32 devices in a mesh: dp: 8 (over y, x, core), mp: 4 (over z).
Axes of the slice: x: 2, y: 2, z: 4, core: 2. Of those that a mesh axis runs over, the one named last changes fastest.
Arguments:
- history_sequences: float32 [64, 512], P('dp'), may hold values from -65 to 65, as said below
- later_steps: float32 [64, 128], P('dp'), may hold values from -65 to 65
- patch_lift_matrix: bfloat16 [32, 1280], P(None, 'dp'), may hold values from -1 to 1
- scaling_factors: bfloat16 [2, 1280], P(None, 'dp'), may hold values from 0.5 to 1.5
- asking_matrix: bfloat16 [1280, 1280], P('dp', 'mp'), may hold values from -0.15625 to 0.15625
- lookup_matrix: bfloat16 [1280, 1280], P('dp', 'mp'), may hold values from -0.15625 to 0.15625
- content_matrix: bfloat16 [1280, 1280], P('dp', 'mp'), may hold values from -0.15625 to 0.15625
- attend_exit_matrix: bfloat16 [1280, 1280], P('mp', 'dp'), may hold values from -0.15625 to 0.15625
- outlook_matrix: bfloat16 [1280, 1280], P('dp', 'mp'), may hold values from -0.15625 to 0.15625
Outputs:
- loss_mean: float32 [], replicated
- embed_grad: float32 [32, 1280], P(None, 'dp')
- gains_grad: float32 [2, 1280], P(None, 'dp')
- query_grad: float32 [1280, 1280], P('dp', 'mp')
- key_grad: float32 [1280, 1280], P('dp', 'mp')
- value_grad: float32 [1280, 1280], P('dp', 'mp')
- output_grad: float32 [1280, 1280], P('mp', 'dp')
- head_weight_gradient: float32 [1280, 1280], P('dp', 'mp')
The draws below stay inside these ranges and needn't reach their ends.
Inputs may be any that keep to these rules, and one draw needn't show every extreme that they name: `history_sequences`: later_steps continues the history of each series.
All inputs are finite; a program needn't handle non-finite values.
Results may differ from the reference program's by a relative error of at most 0.005.
Values may be sent and summed in bfloat16 or wider, within the bound.
A program may use at most 64 MiB of HBM per device.

```python
import math
import jax
import jax.numpy as jnp
from jax import lax

MODEL_WIDTH = 1280
PATCH = 32
HORIZON_SPAN = 128
PATCHES = 16
LEVEL_CHANNELS = 10
HEAD_DIM = 80
PREDICT_COLUMNS = 1280
SERIES = 64
TOKENS = 1024


def history(key):
    total = PATCHES * PATCH + HORIZON_SPAN
    base = jax.random.fold_in(key, 7)
    parts = jax.random.split(base, 5)
    offset_level = 5.0 * jax.random.truncated_normal(parts[0], -3.0, 3.0, (SERIES, 1), dtype=jnp.float32)
    scale = jnp.exp(jax.random.uniform(parts[1], (SERIES, 1), minval=jnp.log(0.3), maxval=jnp.log(10.0)))
    noise = jax.random.truncated_normal(parts[2], -4.0, 4.0, (SERIES, total), dtype=jnp.float32)
    period = jax.random.uniform(parts[3], (SERIES, 1), minval=8.0, maxval=96.0)
    phase = jax.random.uniform(parts[4], (SERIES, 1), minval=0.0, maxval=2.0 * jnp.pi)
    steps = jnp.arange(total, dtype=jnp.float32)[None, :]
    wave = jnp.sin(2.0 * jnp.pi * steps / period + phase)
    return (offset_level + scale * (noise + wave)).astype(jnp.float32)


def draw_history_sequences(key, part):
    return history(key)[:, :PATCHES * PATCH]


def draw_later_steps(key, part):
    return history(key)[:, PATCHES * PATCH:]


def block_levels(key, dims, cuts, least, largest):
    def one(axis_at, blocks):
        steps = jax.random.uniform(jax.random.fold_in(jax.random.fold_in(key, 6), axis_at), (blocks,), jnp.float32, least / len(cuts), largest / len(cuts))
        return jnp.repeat(jnp.exp(steps), dims[axis_at] // blocks).reshape((-1,) + (1,) * (len(dims) - axis_at - 1))

    loudness = one(*cuts[0])
    for cut in cuts[1:]:
        loudness = loudness * one(*cut)
    return loudness


def bell_draw(key, dims, deviation, most, cuts=(), kind=jnp.bfloat16):
    drawn = jax.random.normal(key, dims, jnp.float32) * deviation
    if len(cuts) > 0:
        drawn = block_levels(key, dims, cuts, -0.22, 0.18) * drawn
    return jnp.clip(drawn, min=-most, max=most).astype(kind)


def setup_inputs(seed: int = 0) -> dict:
    seeds = jax.random.split(jax.random.key(seed), 10)
    return {
        "history_sequences": draw_history_sequences(jax.random.fold_in(seeds[9], 71), 0),
        "later_steps": draw_later_steps(jax.random.fold_in(seeds[9], 71), 0),
        "patch_lift_matrix": bell_draw(seeds[2], (PATCH, MODEL_WIDTH), PATCH ** -0.5, 1.0, ((1, 8),)),
        "scaling_factors": jnp.clip(1.0 + 0.1 * jax.random.normal(seeds[3], (2, MODEL_WIDTH), jnp.float32), 0.5, 1.5).astype(jnp.bfloat16),
        "asking_matrix": bell_draw(seeds[4], (MODEL_WIDTH, MODEL_WIDTH), MODEL_WIDTH ** -0.5, 0.15625, ((0, 8), (1, 4))),
        "lookup_matrix": bell_draw(seeds[5], (MODEL_WIDTH, MODEL_WIDTH), MODEL_WIDTH ** -0.5, 0.15625, ((0, 8), (1, 4))),
        "content_matrix": bell_draw(seeds[6], (MODEL_WIDTH, MODEL_WIDTH), MODEL_WIDTH ** -0.5, 0.15625, ((0, 8), (1, 4))),
        "attend_exit_matrix": bell_draw(seeds[7], (MODEL_WIDTH, MODEL_WIDTH), MODEL_WIDTH ** -0.5, 0.15625, ((0, 4), (1, 8))),
        "outlook_matrix": bell_draw(seeds[8], (MODEL_WIDTH, PREDICT_COLUMNS), MODEL_WIDTH ** -0.5, 0.15625, ((0, 8), (1, 4))),
    }


EPS = 1e-06
STAT_EPS = 1e-05
SMOOTHING_RADIUS = 0.05

def rms_forward(residual, gain):
    factor = lax.rsqrt(lax.optimization_barrier(jnp.mean(residual * residual, axis=1, keepdims=True)) + EPS)
    return ((residual * factor * gain[None, :]).astype(jnp.bfloat16), factor)

def rms_backward(residual, factor, gain, upstream):
    weighted = gain[None, :] * upstream
    inner = lax.optimization_barrier(jnp.mean(weighted * residual, axis=1, keepdims=True))
    back = factor * weighted - residual * factor * factor * factor * inner
    gain_term = lax.optimization_barrier(jnp.sum(upstream * residual * factor, axis=0))
    return (back, gain_term)

def positions(length, width):
    half = width // 2
    freqs = jnp.exp(-math.log(10000.0) * jnp.arange(half, dtype=jnp.float32) / half)
    angles = jnp.arange(length, dtype=jnp.float32)[:, None] * freqs[None, :]
    return jnp.concatenate([jnp.sin(angles), jnp.cos(angles)], axis=1)

def prepare(history_sequences, later_steps):
    number = history_sequences.shape[0]
    centre = lax.optimization_barrier(jnp.mean(history_sequences, axis=1, keepdims=True))
    spread = jnp.sqrt(lax.optimization_barrier(jnp.mean((history_sequences - centre) * (history_sequences - centre), axis=1, keepdims=True)) + STAT_EPS)
    normed = (history_sequences - centre) / spread
    ahead = (later_steps - centre) / spread
    joined = jnp.concatenate([normed, ahead], axis=1).reshape(number, -1, PATCH)
    reach = later_steps.shape[1] // PATCH
    future_values = jnp.concatenate([joined[:, offset + 1:offset + 1 + PATCHES] for offset in range(reach)], axis=2)
    future_values = future_values.reshape(number * PATCHES, reach * PATCH)
    patches = normed.reshape(number * PATCHES, PATCH).astype(jnp.bfloat16)
    return (patches, future_values)

def attention_forward(queries, keys, values, number):
    layout = (number, PATCHES, -1, HEAD_DIM)
    query_blocks = queries.reshape(layout).astype(jnp.float32)
    key_blocks = keys.reshape(layout).astype(jnp.float32)
    value_blocks = values.reshape(layout).astype(jnp.float32)
    scale = 1.0 / math.sqrt(HEAD_DIM)
    scores = jnp.einsum('sihd,sjhd->shij', query_blocks, key_blocks) * scale
    place = jnp.arange(PATCHES)
    causal = place[:, None] >= place[None, :]
    raised = jnp.where(causal, jnp.exp(scores), 0.0)
    probs = raised / lax.optimization_barrier(jnp.sum(raised, axis=3, keepdims=True))
    probs_low = probs.astype(jnp.bfloat16)
    context = jnp.einsum('shij,sjhd->sihd', probs_low.astype(jnp.float32), value_blocks)
    context = context.astype(jnp.bfloat16).reshape(number * PATCHES, -1)
    return (context, probs, probs_low)

def attention_backward(context_grad, queries, keys, values, probs, probs_low, number):
    layout = (number, PATCHES, -1, HEAD_DIM)
    query_blocks = queries.reshape(layout).astype(jnp.float32)
    key_blocks = keys.reshape(layout).astype(jnp.float32)
    value_blocks = values.reshape(layout).astype(jnp.float32)
    grad_blocks = context_grad.reshape(layout).astype(jnp.float32)
    scale = 1.0 / math.sqrt(HEAD_DIM)
    prob_grad = jnp.einsum('sihd,sjhd->shij', grad_blocks, value_blocks)
    value_back = jnp.einsum('shij,sihd->sjhd', probs_low.astype(jnp.float32), grad_blocks).astype(jnp.bfloat16)
    centred = prob_grad - lax.optimization_barrier(jnp.sum(probs * prob_grad, axis=3, keepdims=True))
    score_grad = (probs * centred * scale).astype(jnp.bfloat16).astype(jnp.float32)
    query_back = jnp.einsum('shij,sjhd->sihd', score_grad, key_blocks).astype(jnp.bfloat16)
    key_back = jnp.einsum('shij,sihd->sjhd', score_grad, query_blocks).astype(jnp.bfloat16)
    flat = (number * PATCHES, -1)
    return (query_back.reshape(flat), key_back.reshape(flat), value_back.reshape(flat))

def pinball_terms(estimate_entries, actual_entries):
    batch_example_tally = estimate_entries.shape[0]
    horizon_error = actual_entries[:, :, None] - estimate_entries.reshape(batch_example_tally, -1, LEVEL_CHANNELS)
    cumulative_share = jnp.arange(LEVEL_CHANNELS, dtype=jnp.float32) / LEVEL_CHANNELS
    mean_indicator = jnp.arange(LEVEL_CHANNELS) == 0
    lopsided_errors = jnp.where(mean_indicator, horizon_error * horizon_error, cumulative_share * horizon_error + SMOOTHING_RADIUS * jax.nn.softplus(-horizon_error / SMOOTHING_RADIUS))
    skew_coefficient = jnp.where(mean_indicator, -2.0 * horizon_error, jax.nn.sigmoid(-horizon_error / SMOOTHING_RADIUS) - cumulative_share) / HORIZON_SPAN
    return (jnp.sum(lopsided_errors) / HORIZON_SPAN, skew_coefficient.reshape(batch_example_tally, -1).astype(jnp.bfloat16))

def reference(history_sequences, later_steps, patch_lift_matrix, scaling_factors, asking_matrix, lookup_matrix, content_matrix, attend_exit_matrix, outlook_matrix):
    number = history_sequences.shape[0]
    patches, future_values = prepare(history_sequences, later_steps)
    gains = scaling_factors.astype(jnp.float32)
    residual_zero = jnp.dot(patches, patch_lift_matrix, preferred_element_type=jnp.float32) + jnp.tile(positions(PATCHES, MODEL_WIDTH), (number, 1))
    normed_attn, factor_attn = rms_forward(residual_zero, gains[0])
    queries = jnp.dot(normed_attn, asking_matrix, preferred_element_type=jnp.float32).astype(jnp.bfloat16)
    keys = jnp.dot(normed_attn, lookup_matrix, preferred_element_type=jnp.float32).astype(jnp.bfloat16)
    values = jnp.dot(normed_attn, content_matrix, preferred_element_type=jnp.float32).astype(jnp.bfloat16)
    context, probs, probs_low = attention_forward(queries, keys, values, number)
    residual_one = residual_zero + jnp.dot(context, attend_exit_matrix, preferred_element_type=jnp.float32)
    normed_head, factor_head = rms_forward(residual_one, gains[1])
    estimate_entries = jnp.dot(normed_head, outlook_matrix, preferred_element_type=jnp.float32)
    total_loss_value, estimate_derivative = pinball_terms(estimate_entries, future_values)
    loss_mean = total_loss_value / TOKENS
    head_weight_gradient = jnp.dot(normed_head.T, estimate_derivative, preferred_element_type=jnp.float32)
    head_reverse = jnp.dot(estimate_derivative, outlook_matrix.T, preferred_element_type=jnp.float32)
    residual_one_grad, gain_one = rms_backward(residual_one, factor_head, gains[1], head_reverse)
    attn_low = residual_one_grad.astype(jnp.bfloat16)
    output_grad = jnp.dot(context.T, attn_low, preferred_element_type=jnp.float32)
    context_grad = jnp.dot(attn_low, attend_exit_matrix.T, preferred_element_type=jnp.float32).astype(jnp.bfloat16)
    query_back, key_back, value_back = attention_backward(context_grad, queries, keys, values, probs, probs_low, number)
    query_grad = jnp.dot(normed_attn.T, query_back, preferred_element_type=jnp.float32)
    key_grad = jnp.dot(normed_attn.T, key_back, preferred_element_type=jnp.float32)
    value_grad = jnp.dot(normed_attn.T, value_back, preferred_element_type=jnp.float32)
    attn_back = jnp.dot(query_back, asking_matrix.T, preferred_element_type=jnp.float32)
    attn_back = attn_back + jnp.dot(key_back, lookup_matrix.T, preferred_element_type=jnp.float32)
    attn_back = attn_back + jnp.dot(value_back, content_matrix.T, preferred_element_type=jnp.float32)
    norm_back_zero, gain_zero = rms_backward(residual_zero, factor_attn, gains[0], attn_back)
    residual_zero_grad = residual_one_grad + norm_back_zero
    embed_grad = jnp.dot(patches.T, residual_zero_grad.astype(jnp.bfloat16), preferred_element_type=jnp.float32)
    gains_grad = jnp.stack([gain_zero, gain_one], axis=0)
    return (loss_mean, embed_grad, gains_grad, query_grad, key_grad, value_grad, output_grad, head_weight_gradient)
```

```python
import functools
import math

import jax
import jax.numpy as jnp
import numpy as np
from jax import lax
from jax.experimental import pallas as pl
from jax.experimental.pallas import tpu as pltpu
from jax.sharding import PartitionSpec as P

PATCH = 32
HORIZON_SPAN = 128
PATCHES = 16
LEVEL_CHANNELS = 10
HEAD_DIM = 80


EPS = 1e-06
STAT_EPS = 1e-05
SMOOTHING_RADIUS = 0.05


def rms_forward(residual, gain):
    factor = lax.rsqrt(jnp.mean(residual * residual, axis=1, keepdims=True) + EPS)
    return ((residual * factor * gain[None, :]).astype(jnp.bfloat16), factor)


def rms_backward(residual, factor, gain, upstream):
    weighted = gain[None, :] * upstream
    inner = jnp.mean(weighted * residual, axis=1, keepdims=True)
    back = factor * weighted - residual * factor * factor * factor * inner
    gain_term = jnp.sum(upstream * residual * factor, axis=0)
    return (back, gain_term)


def positions(length, width):
    half = width // 2
    freqs = jnp.exp(-math.log(10000.0) * jnp.arange(half, dtype=jnp.float32) / half)
    angles = jnp.arange(length, dtype=jnp.float32)[:, None] * freqs[None, :]
    return jnp.concatenate([jnp.sin(angles), jnp.cos(angles)], axis=1)


def prepare(history_sequences, later_steps):
    number = history_sequences.shape[0]
    centre = jnp.mean(history_sequences, axis=1, keepdims=True)
    spread = jnp.sqrt(
        jnp.mean((history_sequences - centre) * (history_sequences - centre), axis=1, keepdims=True)
        + STAT_EPS
    )
    normed = (history_sequences - centre) / spread
    ahead = (later_steps - centre) / spread
    joined = jnp.concatenate([normed, ahead], axis=1).reshape(number, -1, PATCH)
    reach = later_steps.shape[1] // PATCH
    future_values = jnp.concatenate(
        [joined[:, offset + 1 : offset + 1 + PATCHES] for offset in range(reach)], axis=2
    )
    future_values = future_values.reshape(number * PATCHES, reach * PATCH)
    patches = normed.reshape(number * PATCHES, PATCH).astype(jnp.bfloat16)
    return (patches, future_values)


def attention_forward(queries, keys, values, number):
    layout = (number, PATCHES, -1, HEAD_DIM)
    query_blocks = queries.reshape(layout)
    key_blocks = keys.reshape(layout)
    value_blocks = values.reshape(layout)
    scale = 1.0 / math.sqrt(HEAD_DIM)
    scores = (
        jnp.einsum("sihd,sjhd->shij", query_blocks, key_blocks, preferred_element_type=jnp.float32)
        * scale
    )
    place = jnp.arange(PATCHES)
    causal = place[:, None] >= place[None, :]
    raised = jnp.where(causal, jnp.exp(scores), 0.0)
    probs = raised / jnp.sum(raised, axis=3, keepdims=True)
    probs_low = probs.astype(jnp.bfloat16)
    context = jnp.einsum(
        "shij,sjhd->sihd", probs_low, value_blocks, preferred_element_type=jnp.float32
    )
    context = context.astype(jnp.bfloat16).reshape(number * PATCHES, -1)
    return (context, probs, probs_low)


def attention_backward(context_grad, queries, keys, values, probs, probs_low, number):
    layout = (number, PATCHES, -1, HEAD_DIM)
    query_blocks = queries.reshape(layout)
    key_blocks = keys.reshape(layout)
    value_blocks = values.reshape(layout)
    grad_blocks = context_grad.reshape(layout)
    scale = 1.0 / math.sqrt(HEAD_DIM)
    prob_grad = jnp.einsum(
        "sihd,sjhd->shij", grad_blocks, value_blocks, preferred_element_type=jnp.float32
    )
    value_back = jnp.einsum(
        "shij,sihd->sjhd", probs_low, grad_blocks, preferred_element_type=jnp.float32
    ).astype(jnp.bfloat16)
    centred = prob_grad - jnp.sum(probs * prob_grad, axis=3, keepdims=True)
    score_grad = (probs * centred * scale).astype(jnp.bfloat16)
    query_back = jnp.einsum(
        "shij,sjhd->sihd", score_grad, key_blocks, preferred_element_type=jnp.float32
    ).astype(jnp.bfloat16)
    key_back = jnp.einsum(
        "shij,sihd->sjhd", score_grad, query_blocks, preferred_element_type=jnp.float32
    ).astype(jnp.bfloat16)
    flat = (number * PATCHES, -1)
    return (query_back.reshape(flat), key_back.reshape(flat), value_back.reshape(flat))


def pinball_terms(estimate_entries, actual_entries):
    batch_example_tally = estimate_entries.shape[0]
    horizon_error = actual_entries[:, :, None] - estimate_entries.reshape(
        batch_example_tally, -1, LEVEL_CHANNELS
    )
    cumulative_share = jnp.arange(LEVEL_CHANNELS, dtype=jnp.float32) / LEVEL_CHANNELS
    mean_indicator = jnp.arange(LEVEL_CHANNELS) == 0
    lopsided_errors = jnp.where(
        mean_indicator,
        horizon_error * horizon_error,
        cumulative_share * horizon_error
        + SMOOTHING_RADIUS * jax.nn.softplus(-horizon_error / SMOOTHING_RADIUS),
    )
    skew_coefficient = (
        jnp.where(
            mean_indicator,
            -2.0 * horizon_error,
            jax.nn.sigmoid(-horizon_error / SMOOTHING_RADIUS) - cumulative_share,
        )
        / HORIZON_SPAN
    )
    return (
        jnp.sum(lopsided_errors) / HORIZON_SPAN,
        skew_coefficient.reshape(batch_example_tally, -1).astype(jnp.bfloat16),
    )


def multiplied_rows(left, right):

    def term(start, count):
        return jnp.dot(left, right, preferred_element_type=jnp.float32)

    return term


def per_device(
    history_sequences,
    later_steps,
    patch_lift_matrix,
    scaling_factors,
    asking_matrix,
    lookup_matrix,
    content_matrix,
    attend_exit_matrix,
    outlook_matrix,
):
    number = history_sequences.shape[0]
    rows_all = number * PATCHES
    patches, future_values = prepare(history_sequences, later_steps)
    embed_full, gains_full = (
        lax.all_gather(patch_lift_matrix, "dp", axis=1, tiled=True),
        lax.all_gather(scaling_factors, "dp", axis=1, tiled=True),
    )
    gains = gains_full.astype(jnp.float32)
    query_full, key_full, value_full, outlook_collected = (
        lax.all_gather(asking_matrix, "dp", axis=0, tiled=True),
        lax.all_gather(lookup_matrix, "dp", axis=0, tiled=True),
        lax.all_gather(content_matrix, "dp", axis=0, tiled=True),
        lax.all_gather(outlook_matrix, "dp", axis=0, tiled=True),
    )
    output_full = lax.all_gather(attend_exit_matrix, "dp", axis=1, tiled=True)
    residual_zero = jnp.dot(patches, embed_full, preferred_element_type=jnp.float32) + jnp.tile(
        positions(PATCHES, embed_full.shape[1]), (number, 1)
    )
    normed_attn, factor_attn = rms_forward(residual_zero, gains[0])
    queries = jnp.dot(normed_attn, query_full, preferred_element_type=jnp.float32).astype(
        jnp.bfloat16
    )
    keys = jnp.dot(normed_attn, key_full, preferred_element_type=jnp.float32).astype(jnp.bfloat16)
    values = jnp.dot(normed_attn, value_full, preferred_element_type=jnp.float32).astype(
        jnp.bfloat16
    )
    context, probs, probs_low = attention_forward(queries, keys, values, number)
    attn_term = multiplied_rows(context, output_full)
    residual_one = residual_zero + lax.psum(attn_term(0, rows_all), "mp")
    normed_head, factor_head = rms_forward(residual_one, gains[1])
    estimate_entries = jnp.dot(normed_head, outlook_collected, preferred_element_type=jnp.float32)
    device_portion = estimate_entries.shape[1] // LEVEL_CHANNELS
    actual_entries = lax.dynamic_slice_in_dim(
        future_values, lax.axis_index("mp") * device_portion, device_portion, 1
    )
    device_loss, estimate_derivative = pinball_terms(estimate_entries, actual_entries)
    total_loss_value = lax.psum(device_loss, ("dp", "mp"))
    loss_mean = total_loss_value / (number * PATCHES * lax.axis_size("dp"))
    head_weight_gradient = jnp.dot(
        normed_head.T, estimate_derivative, preferred_element_type=jnp.float32
    )
    head_contribution = multiplied_rows(estimate_derivative, outlook_collected.T)
    head_reverse = lax.psum(head_contribution(0, rows_all).astype(jnp.bfloat16), "mp").astype(
        jnp.float32
    )
    residual_one_grad, gain_one = rms_backward(residual_one, factor_head, gains[1], head_reverse)
    attn_low = residual_one_grad.astype(jnp.bfloat16)
    output_grad = jnp.dot(context.T, attn_low, preferred_element_type=jnp.float32)
    context_grad = jnp.dot(attn_low, output_full.T, preferred_element_type=jnp.float32).astype(
        jnp.bfloat16
    )
    query_back, key_back, value_back = attention_backward(
        context_grad, queries, keys, values, probs, probs_low, number
    )
    query_grad = jnp.dot(normed_attn.T, query_back, preferred_element_type=jnp.float32)
    key_grad = jnp.dot(normed_attn.T, key_back, preferred_element_type=jnp.float32)
    value_grad = jnp.dot(normed_attn.T, value_back, preferred_element_type=jnp.float32)
    total = jnp.dot(query_back, query_full.T, preferred_element_type=jnp.float32)
    total = total + jnp.dot(key_back, key_full.T, preferred_element_type=jnp.float32)
    attn_back = lax.psum(
        (total + jnp.dot(value_back, value_full.T, preferred_element_type=jnp.float32)).astype(
            jnp.bfloat16
        ),
        "mp",
    ).astype(jnp.float32)
    norm_back_zero, gain_zero = rms_backward(residual_zero, factor_attn, gains[0], attn_back)
    residual_zero_grad = residual_one_grad + norm_back_zero
    embed_grad = jnp.dot(
        patches.T, residual_zero_grad.astype(jnp.bfloat16), preferred_element_type=jnp.float32
    )
    gains_grad = jnp.stack([gain_zero, gain_one], axis=0)
    query_grad, key_grad, value_grad, head_weight_gradient = (
        lax.psum_scatter(query_grad, "dp", scatter_dimension=0, tiled=True),
        lax.psum_scatter(key_grad, "dp", scatter_dimension=0, tiled=True),
        lax.psum_scatter(value_grad, "dp", scatter_dimension=0, tiled=True),
        lax.psum_scatter(head_weight_gradient, "dp", scatter_dimension=0, tiled=True),
    )
    output_grad = lax.psum_scatter(output_grad, "dp", scatter_dimension=1, tiled=True)
    embed_grad, gains_grad = (
        lax.psum_scatter(embed_grad, "dp", scatter_dimension=1, tiled=True),
        lax.psum_scatter(gains_grad, "dp", scatter_dimension=1, tiled=True),
    )
    return (
        loss_mean,
        embed_grad,
        gains_grad,
        query_grad,
        key_grad,
        value_grad,
        output_grad,
        head_weight_gradient,
    )


MESH = pl.DeviceIdType.MESH
BF = jnp.bfloat16
F32 = jnp.float32


def mm(left, right, dims=(1, 0)):
    return lax.dot_general(
        left, right, (((dims[0],), (dims[1],)), ((), ())), preferred_element_type=F32
    )


def position_table(length, width):
    half = width // 2
    freqs = np.exp(-math.log(10000.0) * np.arange(half, dtype=np.float32) / np.float32(half))
    angles = np.arange(length, dtype=np.float32)[:, None] * freqs.astype(np.float32)[None, :]
    return np.concatenate([np.sin(angles), np.cos(angles)], axis=1).astype(np.float32)


EG, WQ, WK, WV, WO, WH, CTX, FG, QB, KB, VB = range(11)
NA, NH, AL, EP = range(4)


def sublayer_kernel(
    sizes,
    hist,
    later,
    eg_in,
    wq_in,
    wk_in,
    wv_in,
    wo_in,
    wh_in,
    pos,
    share,
    loss_out,
    eg_out,
    q_out,
    k_out,
    v_out,
    o_out,
    h_out,
    eg_full,
    wq_full,
    wk_full,
    wv_full,
    wo_full,
    wh_full,
    ctx_full,
    fg_full,
    qb_full,
    kb_full,
    vb_full,
    turned,
    na_all,
    nh_all,
    al_all,
    ep_all,
    parts,
    parts_in,
    nh_full,
    al_full,
    rz_ref,
    patch_ref,
    probs_ref,
    egz_own,
    egz_all,
    loss_own,
    loss_dp,
    loss_mid,
    loss_mp,
    ag_send,
    ag_recv,
    xx_send,
    xx_recv,
    z_send,
    z_recv,
    l_send,
    l_recv,
):
    dp, mp = sizes
    chips = dp // 2
    me = lax.axis_index("dp")
    mz = lax.axis_index("mp")
    core = lax.rem(me, 2)
    chip = me // 2
    twin = chip * 2 + 1 - core
    number, steps = hist.shape
    rows = number * PATCHES
    width = pos.shape[1]
    cut = width // dp
    shard = rows // mp
    cols = wq_in.shape[1]
    heads = cols // HEAD_DIM

    def rotated(k):
        return lax.rem(me + k, dp)

    def chip_at(k):
        return lax.rem(chip + k + chips, chips) * 2 + core

    barrier = pltpu.get_barrier_semaphore()
    for k in range(1, dp):
        pl.semaphore_signal(barrier, inc=1, device_id=(rotated(k), mz), device_id_type=MESH)
    for k in range(1, mp):
        pl.semaphore_signal(
            barrier, inc=1, device_id=(me, lax.rem(mz + k, mp)), device_id_type=MESH
        )
    pl.semaphore_wait(barrier, dp - 1 + mp - 1)

    fulls = [
        eg_full, wq_full, wk_full, wv_full, wo_full, wh_full,
        ctx_full, fg_full, qb_full, kb_full, vb_full,
    ]

    def block(full, owner):
        size = full.shape[0] // dp
        return full.at[pl.ds(pl.multiple_of(owner * size, 16), size), :]

    def remote(src, dst, send, recv, device):
        return pltpu.make_async_remote_copy(
            src_ref=src, dst_ref=dst, send_sem=send, recv_sem=recv,
            device_id=device, device_id_type=MESH,
        )

    def ag_copy(i, slot, owner, target, src=None):
        place = block(fulls[i], owner)
        return remote(
            place if src is None else src, place,
            ag_send.at[i, slot], ag_recv.at[i, slot], (target, mz),
        )

    def ag_start(i, src=None):
        for k in range(1, chips):
            ag_copy(i, k, me, chip_at(k), src).start()
        ag_copy(i, 0, me, twin, src).start()

    def ag_finish(i):
        for k in range(1, chips):
            owner = chip_at(-k)
            ag_copy(i, k, owner, twin).wait_recv()
            ag_copy(i, chips - 1 + k, owner, twin).start()
        ag_copy(i, 0, twin, twin).wait_recv()
        for k in range(1, chips):
            other = lax.rem(chip - k + chips, chips) * 2 + 1 - core
            ag_copy(i, chips - 1 + k, other, twin).wait_recv()

    def ag_drain(i, src=None):
        for k in range(1, chips):
            ag_copy(i, k, me, chip_at(k), src).wait_send()
            ag_copy(i, chips - 1 + k, chip_at(-k), twin).wait_send()
        ag_copy(i, 0, me, twin, src).wait_send()

    def store_own(i, value):
        size = fulls[i].shape[0] // dp
        fulls[i][pl.ds(pl.multiple_of(me * size, 16), size), :] = value

    lands = [na_all, nh_all, al_all, ep_all]

    def xx_copy(i, k, sender, target):
        if i == EP:
            dst = ep_all.at[sender]
        else:
            dst = lands[i].at[:, pl.ds(pl.multiple_of(sender * rows, 128), rows)]
        return remote(
            turned.at[i, pl.ds(pl.multiple_of(target * cut, 16), cut), :], dst,
            xx_send.at[i, k], xx_recv.at[i, k], (target, mz),
        )

    def xx_start(i, value):
        turned[i] = value
        for k in range(1, dp):
            xx_copy(i, k, me, rotated(k)).start()
        own = turned[i, pl.ds(pl.multiple_of(me * cut, 16), cut), :]
        if i == EP:
            ep_all[me] = own
        else:
            lands[i][:, pl.ds(pl.multiple_of(me * rows, 128), rows)] = own

    def xx_finish(i):
        for k in range(1, dp):
            xx_copy(i, k, lax.rem(me - k + dp, dp), rotated(k)).wait_recv()

    def xx_drain(i):
        for k in range(1, dp):
            xx_copy(i, k, me, rotated(k)).wait_send()

    def z_at(k):
        return lax.rem(mz + k + mp, mp)

    def rs_copy(i, k, sender, target):
        return remote(
            parts.at[i, pl.ds(pl.multiple_of(target * shard, 16), shard), :],
            parts_in.at[i, sender],
            z_send.at[i, k], z_recv.at[i, k], (me, target),
        )

    def rs_start(i, value):
        parts[i] = value.astype(BF)
        for k in range(1, mp):
            rs_copy(i, k, mz, z_at(k)).start()

    def rs_finish(i):
        total = parts[i, pl.ds(pl.multiple_of(mz * shard, 16), shard), :].astype(F32)
        for k in range(1, mp):
            rs_copy(i, k, z_at(-k), z_at(k)).wait_recv()
            total = total + parts_in[i, z_at(-k)].astype(F32)
        return total

    def zg_copy(i, full, k, owner):
        place = full.at[pl.ds(pl.multiple_of(owner * shard, 16), shard), :]
        return remote(place, place, z_send.at[i, k], z_recv.at[i, k], (me, z_at(k)))

    def zg(i, full, value):
        full[pl.ds(pl.multiple_of(mz * shard, 16), shard), :] = value
        for k in range(1, mp):
            zg_copy(i, full, k, mz).start()

    def zg_finish(i, full):
        for k in range(1, mp):
            zg_copy(i, full, k, z_at(-k)).wait_recv()

    inputs = [eg_in, wq_in, wk_in, wv_in, wo_in, wh_in]
    for i, ref in enumerate(inputs):
        ag_start(i, ref)
    for i, ref in enumerate(inputs):
        store_own(i, ref[...])

    history = hist[...]
    centre = jnp.mean(history, axis=1, keepdims=True)
    spread = jnp.sqrt(
        jnp.mean((history - centre) * (history - centre), axis=1, keepdims=True) + STAT_EPS
    )
    normed = (history - centre) / spread
    ahead = (later[...] - centre) / spread
    joined = jnp.concatenate([normed, ahead], axis=1)
    span = joined.shape[1]
    wide = jnp.broadcast_to(joined[:, None, :], (number, PATCHES, span)).reshape(rows, span)
    row = lax.broadcasted_iota(jnp.int32, (rows, span), 0)
    at = lax.broadcasted_iota(jnp.int32, (rows, span), 1)
    offset = at - PATCH * (row & (PATCHES - 1))
    here = (offset >= 0) & (offset < PATCH)
    lane = lax.broadcasted_iota(jnp.int32, (span, 128), 1)
    low = lax.broadcasted_iota(jnp.int32, (span, 128), 0) & (PATCH - 1)
    fold = jnp.where(lane == low, 1.0, 0.0).astype(BF)
    patches = mm(jnp.where(here, wide, 0.0).astype(BF), fold).astype(BF)
    patch_ref[...] = patches

    portion = cols // LEVEL_CHANNELS
    reach = offset - PATCH - portion * mz
    chosen = jnp.where((reach >= 0) & (reach < portion), wide, 0.0)
    column = lax.broadcasted_iota(jnp.int32, (span, cols), 1)
    first = (lax.broadcasted_iota(jnp.int32, (span, cols), 0) & (PATCH - 1)) * LEVEL_CHANNELS
    spreader = jnp.where((column >= first) & (column < first + LEVEL_CHANNELS), 1.0, 0.0).astype(BF)
    target = jnp.zeros((rows, cols), F32)
    rest = chosen
    for _ in range(3):
        piece = rest.astype(BF)
        target = target + mm(piece, spreader)
        rest = rest - piece.astype(F32)

    ag_finish(EG)
    lifted = eg_full[...]
    table = jnp.broadcast_to(pos[...][None], (number, PATCHES, width)).reshape(rows, width)
    rz = mm(patches, lifted, (1, 1)) + table
    rz_ref[...] = rz
    pick = lax.broadcasted_iota(jnp.int32, (16, 128), 1) - lax.broadcasted_iota(
        jnp.int32, (16, 128), 0
    )
    gains = mm(jnp.where(pick == PATCH, 1.0, 0.0).astype(BF), lifted, (1, 1))
    gain_attn = gains[0:1, :]
    gain_head = gains[1:2, :]
    factor = lax.rsqrt(jnp.mean(rz * rz, axis=1, keepdims=True) + EPS)
    na = rz * factor * gain_attn
    na_low = na.astype(BF)
    xx_start(NA, na.T.astype(BF))

    ag_finish(WQ)
    q = mm(na_low, wq_full[...])
    ag_finish(WK)
    k_ = mm(na_low, wk_full[...])
    ag_finish(WV)
    v = mm(na_low, wv_full[...])
    q_low, k_low, v_low = q.astype(BF), k_.astype(BF), v.astype(BF)

    head_lane = lax.broadcasted_iota(jnp.int32, (1, cols), 1)
    masks = [
        jnp.where((head_lane >= h * HEAD_DIM) & (head_lane < (h + 1) * HEAD_DIM), 1.0, 0.0)
        for h in range(heads)
    ]
    r_at = lax.broadcasted_iota(jnp.int32, (rows, rows), 0)
    c_at = lax.broadcasted_iota(jnp.int32, (rows, rows), 1)
    causal = (c_at <= r_at) & (c_at >= r_at - (r_at & (PATCHES - 1)))
    scale = 1.0 / math.sqrt(HEAD_DIM)
    ctx = jnp.zeros((rows, cols), F32)
    for h in range(heads):
        scores = mm((q * masks[h]).astype(BF), k_low, (1, 1)) * scale
        raised = jnp.where(causal, jnp.exp(scores), 0.0)
        probs = raised / jnp.sum(raised, axis=1, keepdims=True)
        probs_ref[h] = probs
        ctx = ctx + mm(probs.astype(BF), (v * masks[h]).astype(BF))
    ctx_low = ctx.astype(BF)
    store_own(CTX, ctx_low)
    ag_start(CTX)
    ag_finish(WO)
    rs_start(0, mm(ctx_low, wo_full[...], (1, 1)))
    ag_finish(WH)
    shard_rows = pl.ds(pl.multiple_of(mz * shard, 16), shard)
    rz_shard = rz_ref[shard_rows, :]
    r1 = rz_shard + rs_finish(0)
    factor_head = lax.rsqrt(jnp.mean(r1 * r1, axis=1, keepdims=True) + EPS)
    zg(3, nh_full, (r1 * factor_head * gain_head).astype(BF))
    zg_finish(3, nh_full)
    nh = nh_full[...]
    error = target - mm(nh, wh_full[...])
    shares = share[0:1, :]
    is_mean = shares == 0.0
    slope = -error / SMOOTHING_RADIUS
    small = jnp.exp(-jnp.abs(slope))
    soft = jnp.maximum(slope, 0.0) + jnp.log1p(small)
    sig = jnp.where(slope >= 0.0, 1.0, small) / (1.0 + small)
    terms = jnp.where(is_mean, error * error, shares * error + SMOOTHING_RADIUS * soft)
    fg = (jnp.where(is_mean, -2.0 * error, sig - shares) / HORIZON_SPAN).astype(BF)
    store_own(FG, fg)
    ag_start(FG)
    rs_start(1, mm(fg, wh_full[...], (1, 1)))
    xx_start(NH, nh.astype(F32).T.astype(BF))
    loss_here = jnp.sum(jnp.sum(terms, axis=1, keepdims=True), axis=0, keepdims=True)
    loss_own[...] = jnp.broadcast_to(loss_here, loss_own.shape)

    def loss_copy(k, sender):
        return remote(
            loss_own, loss_dp.at[sender], l_send.at[0, k], l_recv.at[0, k], (rotated(k), mz)
        )

    def loss_z(k, sender):
        return remote(
            loss_mid, loss_mp.at[sender], l_send.at[1, k], l_recv.at[1, k], (me, z_at(k))
        )

    for k in range(1, dp):
        loss_copy(k, me).start()
    ag_finish(CTX)

    up = rs_finish(1)
    weighted = gain_head * up
    inner = jnp.mean(weighted * r1, axis=1, keepdims=True)
    r1_grad = factor_head * weighted - r1 * factor_head * factor_head * factor_head * inner
    gain_one = jnp.sum(up * r1 * factor_head, axis=0, keepdims=True)
    zg(4, al_full, r1_grad.astype(BF))
    ag_finish(FG)
    zg_finish(4, al_full)
    al = al_full[...]
    cg = mm(al, wo_full[...])
    qb = jnp.zeros((rows, cols), F32)
    kb = jnp.zeros((rows, cols), F32)
    vb = jnp.zeros((rows, cols), F32)
    for h in range(heads):
        cg_head = (cg * masks[h]).astype(BF)
        probs = probs_ref[h]
        prob_grad = mm(cg_head, v_low, (1, 1))
        vb = vb + mm(probs.T.astype(BF), cg_head)
        centred = prob_grad - jnp.sum(probs * prob_grad, axis=1, keepdims=True)
        score_grad = probs * centred * scale
        qb = qb + mm(score_grad.astype(BF), (k_ * masks[h]).astype(BF))
        kb = kb + mm(score_grad.T.astype(BF), (q * masks[h]).astype(BF))
    qb, kb, vb = qb.astype(BF), kb.astype(BF), vb.astype(BF)
    for i, value in ((QB, qb), (KB, kb), (VB, vb)):
        store_own(i, value)
        ag_start(i)
    back = mm(qb, wq_full[...], (1, 1)) + mm(kb, wk_full[...], (1, 1))
    rs_start(2, back + mm(vb, wv_full[...], (1, 1)))
    xx_start(AL, al.astype(F32).T.astype(BF))

    total = loss_own[...]
    for k in range(1, dp):
        loss_copy(k, lax.rem(me - k + dp, dp)).wait_recv()
        total = total + loss_dp[lax.rem(me - k + dp, dp)]
    loss_mid[...] = total
    for k in range(1, mp):
        loss_z(k, mz).start()
    xx_finish(NH)
    h_out[...] = mm(nh_all[...], fg_full[...])

    up = rs_finish(2)
    factor = lax.rsqrt(jnp.mean(rz_shard * rz_shard, axis=1, keepdims=True) + EPS)
    weighted = gain_attn * up
    inner = jnp.mean(weighted * rz_shard, axis=1, keepdims=True)
    rz_grad = r1_grad + (factor * weighted - rz_shard * factor * factor * factor * inner)
    gain_zero = jnp.sum(up * rz_shard * factor, axis=0, keepdims=True)
    which = lax.broadcasted_iota(jnp.int32, (16, width), 0)
    both = jnp.where(which == 0, gain_zero, jnp.where(which == 1, gain_one, 0.0))
    both_high = both.astype(BF).astype(F32)
    stacked = jnp.concatenate([rz_grad, both_high, both - both_high], axis=0)
    hot = jnp.where(pick == PATCH, 1.0, 0.0)
    other = jnp.concatenate([patch_ref[shard_rows, :].astype(F32), hot, hot], axis=0)
    xx_start(EP, mm(stacked.T.astype(BF), other.astype(BF)).astype(BF))

    total = loss_mid[...]
    for k in range(1, mp):
        loss_z(k, z_at(-k)).wait_recv()
        total = total + loss_mp[z_at(-k)]
    loss_out[...] = total / (number * PATCHES * dp * HORIZON_SPAN)
    for i in (QB, KB, VB):
        ag_finish(i)

    xx_finish(EP)
    summed = ep_all[0].astype(F32)
    for d in range(1, dp):
        summed = summed + ep_all[d].astype(F32)
    egz_own[...] = summed.astype(BF)

    def egz(k, sender):
        return remote(egz_own, egz_all.at[sender], z_send.at[5, k], z_recv.at[5, k], (me, z_at(k)))

    for k in range(1, mp):
        egz(k, mz).start()

    xx_finish(NA)
    na_every = na_all[...]
    q_out[...] = mm(na_every, qb_full[...])
    k_out[...] = mm(na_every, kb_full[...])
    v_out[...] = mm(na_every, vb_full[...])
    xx_finish(AL)
    o_out[...] = mm(al_all[...], ctx_full[...])
    for k in range(1, mp):
        egz(k, z_at(-k)).wait_recv()
        summed = summed + egz_all[z_at(-k)].astype(F32)
    eg_out[...] = summed

    for i in range(len(fulls)):
        ag_drain(i, inputs[i] if i < len(inputs) else None)
    for i in range(4):
        xx_drain(i)
    for k in range(1, dp):
        loss_copy(k, me).wait_send()
    for k in range(1, mp):
        for i in range(3):
            rs_copy(i, k, mz, z_at(k)).wait_send()
        zg_copy(3, nh_full, k, mz).wait_send()
        zg_copy(4, al_full, k, mz).wait_send()
        egz(k, mz).wait_send()
        loss_z(k, mz).wait_send()


def fused_device(
    dp,
    mp,
    history_sequences,
    later_steps,
    patch_lift_matrix,
    scaling_factors,
    asking_matrix,
    lookup_matrix,
    content_matrix,
    attend_exit_matrix,
    outlook_matrix,
):
    number = history_sequences.shape[0]
    rows = number * PATCHES
    cut, cols = asking_matrix.shape
    width = cut * dp
    small = jnp.concatenate([patch_lift_matrix, scaling_factors], axis=0)
    small = jnp.pad(small, ((0, 128 - small.shape[0]), (0, 0))).T
    levels = np.arange(cols) % LEVEL_CHANNELS
    share = np.broadcast_to((levels.astype(np.float32) / LEVEL_CHANNELS)[None], (8, cols))
    vmem = pltpu.VMEM
    full = vmem((width, cols), BF)
    tall = vmem((rows * dp, cols), BF)
    across = vmem((cut, rows * dp), BF)
    dma = pltpu.SemaphoreType.DMA
    grad = jax.ShapeDtypeStruct((cut, cols), F32)
    shard = rows // mp
    chips = dp // 2
    loss, small_grad, query_grad, key_grad, value_grad, output_grad, head_grad = pl.pallas_call(
        functools.partial(sublayer_kernel, (dp, mp)),
        out_shape=(
            jax.ShapeDtypeStruct((8, 128), F32),
            jax.ShapeDtypeStruct((cut, 128), F32),
            grad, grad, grad, grad, grad,
        ),
        in_specs=[pl.BlockSpec(memory_space=vmem)] * 10,
        out_specs=(pl.BlockSpec(memory_space=vmem),) * 7,
        scratch_shapes=[
            vmem((width, 128), BF), full, full, full, full, full,
            tall, tall, tall, tall, tall,
            vmem((4, width, rows), BF),
            across, across, across,
            vmem((dp, cut, rows), BF),
            vmem((3, rows, width), BF),
            vmem((3, mp, shard, width), BF),
            vmem((rows, width), BF),
            vmem((rows, width), BF),
            vmem((rows, width), F32),
            vmem((rows, 128), BF),
            vmem((cols // HEAD_DIM, rows, rows), F32),
            vmem((cut, 128), BF),
            vmem((mp, cut, 128), BF),
            vmem((8, 128), F32),
            vmem((dp, 8, 128), F32),
            vmem((8, 128), F32),
            vmem((mp, 8, 128), F32),
            dma((11, 2 * chips - 1)), dma((11, 2 * chips - 1)),
            dma((4, dp)), dma((4, dp)),
            dma((6, mp)), dma((6, mp)),
            dma((2, max(dp, mp))), dma((2, max(dp, mp))),
        ],
        compiler_params=pltpu.CompilerParams(
            collective_id=0, has_side_effects=True, vmem_limit_bytes=56 * 1024 * 1024
        ),
    )(
        history_sequences, later_steps, small, asking_matrix, lookup_matrix, content_matrix,
        attend_exit_matrix.T, outlook_matrix,
        jnp.asarray(position_table(PATCHES, width)), jnp.asarray(share),
    )
    lift = patch_lift_matrix.shape[0]
    gains = scaling_factors.shape[0]
    return (
        loss[0, 0],
        small_grad[:, :lift].T,
        small_grad[:, lift : lift + gains].T,
        query_grad,
        key_grad,
        value_grad,
        output_grad.T,
        head_grad,
    )


def fits(dp, mp, arrays):
    rows = arrays[0].shape[0] * PATCHES
    cut, cols = arrays[4].shape
    return (
        rows == 128
        and dp % 2 == 0
        and dp > 2
        and mp > 1
        and cut % 16 == 0
        and rows % (16 * mp) == 0
        and cols % HEAD_DIM == 0
        and cols == PATCH * LEVEL_CHANNELS
    )


def solution(mesh):
    in_specs = (
        P("dp", None),
        P("dp", None),
        P(None, "dp"),
        P(None, "dp"),
        P("dp", "mp"),
        P("dp", "mp"),
        P("dp", "mp"),
        P("mp", "dp"),
        P("dp", "mp"),
    )
    out_specs = (
        P(),
        P(None, "dp"),
        P(None, "dp"),
        P("dp", "mp"),
        P("dp", "mp"),
        P("dp", "mp"),
        P("mp", "dp"),
        P("dp", "mp"),
    )
    dp, mp = mesh.shape["dp"], mesh.shape["mp"]

    def step(*arrays):
        if fits(dp, mp, arrays):
            return fused_device(dp, mp, *arrays)
        return per_device(*arrays)

    return jax.shard_map(
        step, mesh=mesh, in_specs=in_specs, out_specs=out_specs, check_vma=False
    )
```

```python
import functools
import math

import jax
import jax.numpy as jnp
import numpy as np
from jax import lax
from jax.experimental import pallas as pl
from jax.experimental.pallas import tpu as pltpu
from jax.sharding import PartitionSpec as P

PATCH = 32
HORIZON_SPAN = 128
PATCHES = 16
LEVEL_CHANNELS = 10
HEAD_DIM = 80


EPS = 1e-06
STAT_EPS = 1e-05
SMOOTHING_RADIUS = 0.05


def rms_forward(residual, gain):
    factor = lax.rsqrt(jnp.mean(residual * residual, axis=1, keepdims=True) + EPS)
    return ((residual * factor * gain[None, :]).astype(jnp.bfloat16), factor)


def rms_backward(residual, factor, gain, upstream):
    weighted = gain[None, :] * upstream
    inner = jnp.mean(weighted * residual, axis=1, keepdims=True)
    back = factor * weighted - residual * factor * factor * factor * inner
    gain_term = jnp.sum(upstream * residual * factor, axis=0)
    return (back, gain_term)


def positions(length, width):
    half = width // 2
    freqs = jnp.exp(-math.log(10000.0) * jnp.arange(half, dtype=jnp.float32) / half)
    angles = jnp.arange(length, dtype=jnp.float32)[:, None] * freqs[None, :]
    return jnp.concatenate([jnp.sin(angles), jnp.cos(angles)], axis=1)


def prepare(history_sequences, later_steps):
    number = history_sequences.shape[0]
    centre = jnp.mean(history_sequences, axis=1, keepdims=True)
    spread = jnp.sqrt(
        jnp.mean((history_sequences - centre) * (history_sequences - centre), axis=1, keepdims=True)
        + STAT_EPS
    )
    normed = (history_sequences - centre) / spread
    ahead = (later_steps - centre) / spread
    joined = jnp.concatenate([normed, ahead], axis=1).reshape(number, -1, PATCH)
    reach = later_steps.shape[1] // PATCH
    future_values = jnp.concatenate(
        [joined[:, offset + 1 : offset + 1 + PATCHES] for offset in range(reach)], axis=2
    )
    future_values = future_values.reshape(number * PATCHES, reach * PATCH)
    patches = normed.reshape(number * PATCHES, PATCH).astype(jnp.bfloat16)
    return (patches, future_values)


def attention_forward(queries, keys, values, number):
    layout = (number, PATCHES, -1, HEAD_DIM)
    query_blocks = queries.reshape(layout)
    key_blocks = keys.reshape(layout)
    value_blocks = values.reshape(layout)
    scale = 1.0 / math.sqrt(HEAD_DIM)
    scores = (
        jnp.einsum("sihd,sjhd->shij", query_blocks, key_blocks, preferred_element_type=jnp.float32)
        * scale
    )
    place = jnp.arange(PATCHES)
    causal = place[:, None] >= place[None, :]
    raised = jnp.where(causal, jnp.exp(scores), 0.0)
    probs = raised / jnp.sum(raised, axis=3, keepdims=True)
    probs_low = probs.astype(jnp.bfloat16)
    context = jnp.einsum(
        "shij,sjhd->sihd", probs_low, value_blocks, preferred_element_type=jnp.float32
    )
    context = context.astype(jnp.bfloat16).reshape(number * PATCHES, -1)
    return (context, probs, probs_low)


def attention_backward(context_grad, queries, keys, values, probs, probs_low, number):
    layout = (number, PATCHES, -1, HEAD_DIM)
    query_blocks = queries.reshape(layout)
    key_blocks = keys.reshape(layout)
    value_blocks = values.reshape(layout)
    grad_blocks = context_grad.reshape(layout)
    scale = 1.0 / math.sqrt(HEAD_DIM)
    prob_grad = jnp.einsum(
        "sihd,sjhd->shij", grad_blocks, value_blocks, preferred_element_type=jnp.float32
    )
    value_back = jnp.einsum(
        "shij,sihd->sjhd", probs_low, grad_blocks, preferred_element_type=jnp.float32
    ).astype(jnp.bfloat16)
    centred = prob_grad - jnp.sum(probs * prob_grad, axis=3, keepdims=True)
    score_grad = (probs * centred * scale).astype(jnp.bfloat16)
    query_back = jnp.einsum(
        "shij,sjhd->sihd", score_grad, key_blocks, preferred_element_type=jnp.float32
    ).astype(jnp.bfloat16)
    key_back = jnp.einsum(
        "shij,sihd->sjhd", score_grad, query_blocks, preferred_element_type=jnp.float32
    ).astype(jnp.bfloat16)
    flat = (number * PATCHES, -1)
    return (query_back.reshape(flat), key_back.reshape(flat), value_back.reshape(flat))


def pinball_terms(estimate_entries, actual_entries):
    batch_example_tally = estimate_entries.shape[0]
    horizon_error = actual_entries[:, :, None] - estimate_entries.reshape(
        batch_example_tally, -1, LEVEL_CHANNELS
    )
    cumulative_share = jnp.arange(LEVEL_CHANNELS, dtype=jnp.float32) / LEVEL_CHANNELS
    mean_indicator = jnp.arange(LEVEL_CHANNELS) == 0
    lopsided_errors = jnp.where(
        mean_indicator,
        horizon_error * horizon_error,
        cumulative_share * horizon_error
        + SMOOTHING_RADIUS * jax.nn.softplus(-horizon_error / SMOOTHING_RADIUS),
    )
    skew_coefficient = (
        jnp.where(
            mean_indicator,
            -2.0 * horizon_error,
            jax.nn.sigmoid(-horizon_error / SMOOTHING_RADIUS) - cumulative_share,
        )
        / HORIZON_SPAN
    )
    return (
        jnp.sum(lopsided_errors) / HORIZON_SPAN,
        skew_coefficient.reshape(batch_example_tally, -1).astype(jnp.bfloat16),
    )


def multiplied_rows(left, right):

    def term(start, count):
        return jnp.dot(left, right, preferred_element_type=jnp.float32)

    return term


def per_device(
    history_sequences,
    later_steps,
    patch_lift_matrix,
    scaling_factors,
    asking_matrix,
    lookup_matrix,
    content_matrix,
    attend_exit_matrix,
    outlook_matrix,
):
    number = history_sequences.shape[0]
    rows_all = number * PATCHES
    patches, future_values = prepare(history_sequences, later_steps)
    embed_full, gains_full = (
        lax.all_gather(patch_lift_matrix, "dp", axis=1, tiled=True),
        lax.all_gather(scaling_factors, "dp", axis=1, tiled=True),
    )
    gains = gains_full.astype(jnp.float32)
    query_full, key_full, value_full, outlook_collected = (
        lax.all_gather(asking_matrix, "dp", axis=0, tiled=True),
        lax.all_gather(lookup_matrix, "dp", axis=0, tiled=True),
        lax.all_gather(content_matrix, "dp", axis=0, tiled=True),
        lax.all_gather(outlook_matrix, "dp", axis=0, tiled=True),
    )
    output_full = lax.all_gather(attend_exit_matrix, "dp", axis=1, tiled=True)
    residual_zero = jnp.dot(patches, embed_full, preferred_element_type=jnp.float32) + jnp.tile(
        positions(PATCHES, embed_full.shape[1]), (number, 1)
    )
    normed_attn, factor_attn = rms_forward(residual_zero, gains[0])
    queries = jnp.dot(normed_attn, query_full, preferred_element_type=jnp.float32).astype(
        jnp.bfloat16
    )
    keys = jnp.dot(normed_attn, key_full, preferred_element_type=jnp.float32).astype(jnp.bfloat16)
    values = jnp.dot(normed_attn, value_full, preferred_element_type=jnp.float32).astype(
        jnp.bfloat16
    )
    context, probs, probs_low = attention_forward(queries, keys, values, number)
    attn_term = multiplied_rows(context, output_full)
    residual_one = residual_zero + lax.psum(attn_term(0, rows_all), "mp")
    normed_head, factor_head = rms_forward(residual_one, gains[1])
    estimate_entries = jnp.dot(normed_head, outlook_collected, preferred_element_type=jnp.float32)
    device_portion = estimate_entries.shape[1] // LEVEL_CHANNELS
    actual_entries = lax.dynamic_slice_in_dim(
        future_values, lax.axis_index("mp") * device_portion, device_portion, 1
    )
    device_loss, estimate_derivative = pinball_terms(estimate_entries, actual_entries)
    total_loss_value = lax.psum(device_loss, ("dp", "mp"))
    loss_mean = total_loss_value / (number * PATCHES * lax.axis_size("dp"))
    head_weight_gradient = jnp.dot(
        normed_head.T, estimate_derivative, preferred_element_type=jnp.float32
    )
    head_contribution = multiplied_rows(estimate_derivative, outlook_collected.T)
    head_reverse = lax.psum(head_contribution(0, rows_all).astype(jnp.bfloat16), "mp").astype(
        jnp.float32
    )
    residual_one_grad, gain_one = rms_backward(residual_one, factor_head, gains[1], head_reverse)
    attn_low = residual_one_grad.astype(jnp.bfloat16)
    output_grad = jnp.dot(context.T, attn_low, preferred_element_type=jnp.float32)
    context_grad = jnp.dot(attn_low, output_full.T, preferred_element_type=jnp.float32).astype(
        jnp.bfloat16
    )
    query_back, key_back, value_back = attention_backward(
        context_grad, queries, keys, values, probs, probs_low, number
    )
    query_grad = jnp.dot(normed_attn.T, query_back, preferred_element_type=jnp.float32)
    key_grad = jnp.dot(normed_attn.T, key_back, preferred_element_type=jnp.float32)
    value_grad = jnp.dot(normed_attn.T, value_back, preferred_element_type=jnp.float32)
    total = jnp.dot(query_back, query_full.T, preferred_element_type=jnp.float32)
    total = total + jnp.dot(key_back, key_full.T, preferred_element_type=jnp.float32)
    attn_back = lax.psum(
        (total + jnp.dot(value_back, value_full.T, preferred_element_type=jnp.float32)).astype(
            jnp.bfloat16
        ),
        "mp",
    ).astype(jnp.float32)
    norm_back_zero, gain_zero = rms_backward(residual_zero, factor_attn, gains[0], attn_back)
    residual_zero_grad = residual_one_grad + norm_back_zero
    embed_grad = jnp.dot(
        patches.T, residual_zero_grad.astype(jnp.bfloat16), preferred_element_type=jnp.float32
    )
    gains_grad = jnp.stack([gain_zero, gain_one], axis=0)
    query_grad, key_grad, value_grad, head_weight_gradient = (
        lax.psum_scatter(query_grad, "dp", scatter_dimension=0, tiled=True),
        lax.psum_scatter(key_grad, "dp", scatter_dimension=0, tiled=True),
        lax.psum_scatter(value_grad, "dp", scatter_dimension=0, tiled=True),
        lax.psum_scatter(head_weight_gradient, "dp", scatter_dimension=0, tiled=True),
    )
    output_grad = lax.psum_scatter(output_grad, "dp", scatter_dimension=1, tiled=True)
    embed_grad, gains_grad = (
        lax.psum_scatter(embed_grad, "dp", scatter_dimension=1, tiled=True),
        lax.psum_scatter(gains_grad, "dp", scatter_dimension=1, tiled=True),
    )
    return (
        loss_mean,
        embed_grad,
        gains_grad,
        query_grad,
        key_grad,
        value_grad,
        output_grad,
        head_weight_gradient,
    )


MESH = pl.DeviceIdType.MESH
BF = jnp.bfloat16
F32 = jnp.float32


def mm(left, right, dims=(1, 0)):
    return lax.dot_general(
        left, right, (((dims[0],), (dims[1],)), ((), ())), preferred_element_type=F32
    )


def position_table(length, width):
    half = width // 2
    freqs = np.exp(-math.log(10000.0) * np.arange(half, dtype=np.float32) / np.float32(half))
    angles = np.arange(length, dtype=np.float32)[:, None] * freqs.astype(np.float32)[None, :]
    return np.concatenate([np.sin(angles), np.cos(angles)], axis=1).astype(np.float32)


EG, WQ, WK, WV, WO, WH, CTX, FG, QB, KB, VB = range(11)
NA, NH, AL, EP = range(4)


def sublayer_kernel(
    sizes,
    hist,
    later,
    eg_in,
    wq_in,
    wk_in,
    wv_in,
    wo_in,
    wh_in,
    pos,
    loss_out,
    eg_out,
    q_out,
    k_out,
    v_out,
    o_out,
    h_out,
    eg_full,
    wq_full,
    wk_full,
    wv_full,
    wo_full,
    wh_full,
    ctx_full,
    fg_full,
    qb_full,
    kb_full,
    vb_full,
    turned,
    na_all,
    nh_all,
    al_all,
    ep_all,
    parts,
    parts_in,
    nh_full,
    al_full,
    rz_ref,
    patch_ref,
    probs_ref,
    egz_own,
    egz_all,
    loss_own,
    loss_dp,
    loss_mid,
    loss_mp,
    ag_send,
    ag_recv,
    xx_send,
    xx_recv,
    z_send,
    z_recv,
    l_send,
    l_recv,
):
    dp, mp = sizes
    chips = dp // 2
    me = lax.axis_index("dp")
    mz = lax.axis_index("mp")
    core = lax.rem(me, 2)
    chip = me // 2
    twin = chip * 2 + 1 - core
    number, steps = hist.shape
    rows = number * PATCHES
    width = pos.shape[1]
    cut = width // dp
    half = rows // 2
    shard = half // mp
    cols = wq_in.shape[1]
    heads = cols // HEAD_DIM

    def rotated(k):
        return lax.rem(me + k, dp)

    def chip_at(k):
        return lax.rem(chip + k + chips, chips) * 2 + core

    barrier = pltpu.get_barrier_semaphore()
    for k in range(1, dp):
        pl.semaphore_signal(barrier, inc=1, device_id=(rotated(k), mz), device_id_type=MESH)
    for k in range(1, mp):
        pl.semaphore_signal(
            barrier, inc=1, device_id=(me, lax.rem(mz + k, mp)), device_id_type=MESH
        )
    pl.semaphore_wait(barrier, dp - 1 + mp - 1)

    fulls = [
        eg_full, wq_full, wk_full, wv_full, wo_full, wh_full,
        ctx_full, fg_full, qb_full, kb_full, vb_full,
    ]

    def block(full, owner):
        size = full.shape[0] // dp
        return full.at[pl.ds(pl.multiple_of(owner * size, 16), size), :]

    def remote(src, dst, send, recv, device):
        return pltpu.make_async_remote_copy(
            src_ref=src, dst_ref=dst, send_sem=send, recv_sem=recv,
            device_id=device, device_id_type=MESH,
        )

    def ag_copy(i, slot, owner, target, src=None):
        place = block(fulls[i], owner)
        return remote(
            place if src is None else src, place,
            ag_send.at[i, slot], ag_recv.at[i, slot], (target, mz),
        )

    def ag_start(i, src=None):
        for k in range(1, chips):
            ag_copy(i, k, me, chip_at(k), src).start()
        ag_copy(i, 0, me, twin, src).start()

    def ag_finish(i):
        for k in range(1, chips):
            owner = chip_at(-k)
            ag_copy(i, k, owner, twin).wait_recv()
            ag_copy(i, chips - 1 + k, owner, twin).start()
        ag_copy(i, 0, twin, twin).wait_recv()
        for k in range(1, chips):
            other = lax.rem(chip - k + chips, chips) * 2 + 1 - core
            ag_copy(i, chips - 1 + k, other, twin).wait_recv()

    def ag_drain(i, src=None):
        for k in range(1, chips):
            ag_copy(i, k, me, chip_at(k), src).wait_send()
            ag_copy(i, chips - 1 + k, chip_at(-k), twin).wait_send()
        ag_copy(i, 0, me, twin, src).wait_send()

    def store_own(i, value):
        size = fulls[i].shape[0] // dp
        fulls[i][pl.ds(pl.multiple_of(me * size, 16), size), :] = value

    lands = [na_all, nh_all, al_all, ep_all]

    def xx_copy(i, k, sender, target):
        if i == EP:
            dst = ep_all.at[sender]
        else:
            dst = lands[i].at[:, pl.ds(pl.multiple_of(sender * rows, 128), rows)]
        return remote(
            turned.at[i, pl.ds(pl.multiple_of(target * cut, 16), cut), :], dst,
            xx_send.at[i, k], xx_recv.at[i, k], (target, mz),
        )

    def xx_start(i, value):
        turned[i] = value
        for k in range(1, dp):
            xx_copy(i, k, me, rotated(k)).start()
        own = turned[i, pl.ds(pl.multiple_of(me * cut, 16), cut), :]
        if i == EP:
            ep_all[me] = own
        else:
            lands[i][:, pl.ds(pl.multiple_of(me * rows, 128), rows)] = own

    def xx_finish(i):
        for k in range(1, dp):
            xx_copy(i, k, lax.rem(me - k + dp, dp), rotated(k)).wait_recv()

    def xx_drain(i):
        for k in range(1, dp):
            xx_copy(i, k, me, rotated(k)).wait_send()

    def z_at(k):
        return lax.rem(mz + k + mp, mp)

    def rs_copy(i, k, sender, target):
        return remote(
            parts.at[i, pl.ds(pl.multiple_of(target * shard, 16), shard), :],
            parts_in.at[i, sender],
            z_send.at[i, k], z_recv.at[i, k], (me, target),
        )

    def rs_start(i, value):
        parts[i] = value.astype(BF)
        for k in range(1, mp):
            rs_copy(i, k, mz, z_at(k)).start()

    def rs_finish(i):
        total = parts[i, pl.ds(pl.multiple_of(mz * shard, 16), shard), :].astype(F32)
        for k in range(1, mp):
            rs_copy(i, k, z_at(-k), z_at(k)).wait_recv()
            total = total + parts_in[i, z_at(-k)].astype(F32)
        return total

    def held(b, owner):
        return pl.ds(pl.multiple_of(b * half + owner * shard, 16), shard)

    def zg_copy(i, full, b, k, owner):
        place = full.at[held(b, owner), :]
        return remote(place, place, z_send.at[i, k], z_recv.at[i, k], (me, z_at(k)))

    def zg(i, full, b, value):
        full[held(b, mz), :] = value
        for k in range(1, mp):
            zg_copy(i, full, b, k, mz).start()

    def zg_finish(i, full, b):
        for k in range(1, mp):
            zg_copy(i, full, b, k, z_at(-k)).wait_recv()
        return full[b * half : (b + 1) * half, :]

    inputs = [eg_in, wq_in, wk_in, wv_in, wo_in, wh_in]
    for i, ref in enumerate(inputs):
        ag_start(i, ref)
    for i, ref in enumerate(inputs):
        store_own(i, ref[...])

    history = hist[...]
    centre = jnp.mean(history, axis=1, keepdims=True)
    spread = jnp.sqrt(
        jnp.mean((history - centre) * (history - centre), axis=1, keepdims=True) + STAT_EPS
    )
    normed = (history - centre) / spread
    ahead = (later[...] - centre) / spread
    joined = jnp.concatenate([normed, ahead], axis=1)
    span = joined.shape[1]
    wide = jnp.broadcast_to(joined[:, None, :], (number, PATCHES, span)).reshape(rows, span)
    row = lax.broadcasted_iota(jnp.int32, (rows, span), 0)
    at = lax.broadcasted_iota(jnp.int32, (rows, span), 1)
    offset = at - PATCH * (row & (PATCHES - 1))
    here = (offset >= 0) & (offset < PATCH)
    lane = lax.broadcasted_iota(jnp.int32, (span, 128), 1)
    low = lax.broadcasted_iota(jnp.int32, (span, 128), 0) & (PATCH - 1)
    fold = jnp.where(lane == low, 1.0, 0.0).astype(BF)
    patches = mm(jnp.where(here, wide, 0.0).astype(BF), fold).astype(BF)
    patch_ref[...] = patches

    portion = cols // LEVEL_CHANNELS
    reach = offset - PATCH - portion * mz
    chosen = jnp.where((reach >= 0) & (reach < portion), wide, 0.0)
    column = lax.broadcasted_iota(jnp.int32, (span, cols), 1)
    first = (lax.broadcasted_iota(jnp.int32, (span, cols), 0) & (PATCH - 1)) * LEVEL_CHANNELS
    spreader = jnp.where((column >= first) & (column < first + LEVEL_CHANNELS), 1.0, 0.0).astype(BF)
    target = jnp.zeros((rows, cols), F32)
    rest = chosen
    for _ in range(3):
        piece = rest.astype(BF)
        target = target + mm(piece, spreader)
        rest = rest - piece.astype(F32)

    ag_finish(EG)
    lifted = eg_full[...]
    table = jnp.broadcast_to(pos[...][None], (number, PATCHES, width)).reshape(rows, width)
    rz = mm(patches, lifted, (1, 1)) + table
    rz_ref[...] = rz
    pick = lax.broadcasted_iota(jnp.int32, (16, 128), 1) - lax.broadcasted_iota(
        jnp.int32, (16, 128), 0
    )
    gains = mm(jnp.where(pick == PATCH, 1.0, 0.0).astype(BF), lifted, (1, 1))
    gain_attn = gains[0:1, :]
    gain_head = gains[1:2, :]
    factor = lax.rsqrt(jnp.mean(rz * rz, axis=1, keepdims=True) + EPS)
    na = rz * factor * gain_attn
    na_low = na.astype(BF)
    xx_start(NA, na.T.astype(BF))

    ag_finish(WQ)
    q = mm(na_low, wq_full[...])
    ag_finish(WK)
    k_ = mm(na_low, wk_full[...])
    ag_finish(WV)
    v = mm(na_low, wv_full[...])
    q_low, k_low, v_low = q.astype(BF), k_.astype(BF), v.astype(BF)

    head_lane = lax.broadcasted_iota(jnp.int32, (1, cols), 1)
    masks = [
        jnp.where((head_lane >= h * HEAD_DIM) & (head_lane < (h + 1) * HEAD_DIM), 1.0, 0.0)
        for h in range(heads)
    ]
    r_at = lax.broadcasted_iota(jnp.int32, (half, half), 0)
    c_at = lax.broadcasted_iota(jnp.int32, (half, half), 1)
    causal = (c_at <= r_at) & (c_at >= r_at - (r_at & (PATCHES - 1)))
    scale = 1.0 / math.sqrt(HEAD_DIM)
    spans = [slice(b * half, (b + 1) * half) for b in range(2)]
    contexts = []
    for b, span_b in enumerate(spans):
        ctx = jnp.zeros((half, cols), F32)
        for h in range(heads):
            q_head = (q[span_b] * masks[h]).astype(BF)
            scores = mm(q_head, k_low[span_b], (1, 1)) * scale
            raised = jnp.where(causal, jnp.exp(scores), 0.0)
            probs = raised / jnp.sum(raised, axis=1, keepdims=True)
            probs_ref[b, h] = probs
            ctx = ctx + mm(probs.astype(BF), (v[span_b] * masks[h]).astype(BF))
        contexts.append(ctx.astype(BF))
        if b == 0:
            ag_finish(WO)
        rs_start(b, mm(contexts[b], wo_full[...], (1, 1)))
    store_own(CTX, jnp.concatenate(contexts, axis=0))
    ag_start(CTX)
    ag_finish(WH)
    rz_shards, r1s, factors = [], [], []
    for b in range(2):
        rz_shards.append(rz_ref[held(b, mz), :])
        r1 = rz_shards[b] + rs_finish(b)
        factor_head = lax.rsqrt(jnp.mean(r1 * r1, axis=1, keepdims=True) + EPS)
        zg(6 + b, nh_full, b, (r1 * factor_head * gain_head).astype(BF))
        r1s.append(r1)
        factors.append(factor_head)
    level = lax.broadcasted_iota(jnp.int32, (1, cols), 1).astype(F32)
    level = level - LEVEL_CHANNELS * jnp.floor((level + 0.5) / LEVEL_CHANNELS)
    shares = level / LEVEL_CHANNELS
    is_mean = shares == 0.0
    terms = jnp.zeros((half, cols), F32)
    slopes = []
    for b, span_b in enumerate(spans):
        nh = zg_finish(6 + b, nh_full, b)
        error = target[span_b] - mm(nh, wh_full[...])
        slope = -error / SMOOTHING_RADIUS
        small = jnp.exp(-jnp.abs(slope))
        soft = jnp.maximum(slope, 0.0) + jnp.log1p(small)
        sig = jnp.where(slope >= 0.0, 1.0, small) / (1.0 + small)
        terms = terms + jnp.where(
            is_mean, error * error, shares * error + SMOOTHING_RADIUS * soft
        )
        fg = (jnp.where(is_mean, -2.0 * error, sig - shares) / HORIZON_SPAN).astype(BF)
        slopes.append(fg)
        rs_start(2 + b, mm(fg, wh_full[...], (1, 1)))
    store_own(FG, jnp.concatenate(slopes, axis=0))
    ag_start(FG)
    xx_start(NH, nh_full[...].astype(F32).T.astype(BF))
    loss_here = jnp.sum(jnp.sum(terms, axis=1, keepdims=True), axis=0, keepdims=True)
    loss_own[...] = jnp.broadcast_to(loss_here, loss_own.shape)

    def loss_copy(k, sender):
        return remote(
            loss_own, loss_dp.at[sender], l_send.at[0, k], l_recv.at[0, k], (rotated(k), mz)
        )

    def loss_z(k, sender):
        return remote(
            loss_mid, loss_mp.at[sender], l_send.at[1, k], l_recv.at[1, k], (me, z_at(k))
        )

    for k in range(1, dp):
        loss_copy(k, me).start()
    ag_finish(CTX)

    r1_grads = []
    gain_one = jnp.zeros((1, width), F32)
    for b in range(2):
        up = rs_finish(2 + b)
        r1, factor_head = r1s[b], factors[b]
        weighted = gain_head * up
        inner = jnp.mean(weighted * r1, axis=1, keepdims=True)
        r1_grad = factor_head * weighted - r1 * factor_head * factor_head * factor_head * inner
        zg(8 + b, al_full, b, r1_grad.astype(BF))
        r1_grads.append(r1_grad)
        gain_one = gain_one + jnp.sum(up * r1 * factor_head, axis=0, keepdims=True)
    ag_finish(FG)
    backs = []
    for b, span_b in enumerate(spans):
        cg = mm(zg_finish(8 + b, al_full, b), wo_full[...])
        qb = jnp.zeros((half, cols), F32)
        kb = jnp.zeros((half, cols), F32)
        vb = jnp.zeros((half, cols), F32)
        for h in range(heads):
            cg_head = (cg * masks[h]).astype(BF)
            probs = probs_ref[b, h]
            prob_grad = mm(cg_head, v_low[span_b], (1, 1))
            vb = vb + mm(probs.T.astype(BF), cg_head)
            centred = prob_grad - jnp.sum(probs * prob_grad, axis=1, keepdims=True)
            score_grad = probs * centred * scale
            qb = qb + mm(score_grad.astype(BF), (k_[span_b] * masks[h]).astype(BF))
            kb = kb + mm(score_grad.T.astype(BF), (q[span_b] * masks[h]).astype(BF))
        qb, kb, vb = qb.astype(BF), kb.astype(BF), vb.astype(BF)
        backs.append((qb, kb, vb))
        back = mm(qb, wq_full[...], (1, 1)) + mm(kb, wk_full[...], (1, 1))
        rs_start(4 + b, back + mm(vb, wv_full[...], (1, 1)))
    for n, i in enumerate((QB, KB, VB)):
        store_own(i, jnp.concatenate([backs[0][n], backs[1][n]], axis=0))
        ag_start(i)
    xx_start(AL, al_full[...].astype(F32).T.astype(BF))

    total = loss_own[...]
    for k in range(1, dp):
        loss_copy(k, lax.rem(me - k + dp, dp)).wait_recv()
        total = total + loss_dp[lax.rem(me - k + dp, dp)]
    loss_mid[...] = total
    for k in range(1, mp):
        loss_z(k, mz).start()
    xx_finish(NH)
    h_out[...] = mm(nh_all[...], fg_full[...])

    rz_grads = []
    gain_zero = jnp.zeros((1, width), F32)
    for b in range(2):
        up = rs_finish(4 + b)
        rz_shard = rz_shards[b]
        factor = lax.rsqrt(jnp.mean(rz_shard * rz_shard, axis=1, keepdims=True) + EPS)
        weighted = gain_attn * up
        inner = jnp.mean(weighted * rz_shard, axis=1, keepdims=True)
        rz_grads.append(
            r1_grads[b] + (factor * weighted - rz_shard * factor * factor * factor * inner)
        )
        gain_zero = gain_zero + jnp.sum(up * rz_shard * factor, axis=0, keepdims=True)
    which = lax.broadcasted_iota(jnp.int32, (16, width), 0)
    both = jnp.where(which == 0, gain_zero, jnp.where(which == 1, gain_one, 0.0))
    both_high = both.astype(BF).astype(F32)
    stacked = jnp.concatenate([*rz_grads, both_high, both - both_high], axis=0)
    hot = jnp.where(pick == PATCH, 1.0, 0.0)
    mine = [patch_ref[held(b, mz), :].astype(F32) for b in range(2)]
    other = jnp.concatenate([*mine, hot, hot], axis=0)
    xx_start(EP, mm(stacked.T.astype(BF), other.astype(BF)).astype(BF))

    total = loss_mid[...]
    for k in range(1, mp):
        loss_z(k, z_at(-k)).wait_recv()
        total = total + loss_mp[z_at(-k)]
    loss_out[...] = total / (number * PATCHES * dp * HORIZON_SPAN)
    for i in (QB, KB, VB):
        ag_finish(i)

    xx_finish(EP)
    summed = ep_all[0].astype(F32)
    for d in range(1, dp):
        summed = summed + ep_all[d].astype(F32)
    egz_own[...] = summed.astype(BF)

    def egz(k, sender):
        return remote(egz_own, egz_all.at[sender], z_send.at[10, k], z_recv.at[10, k], (me, z_at(k)))

    for k in range(1, mp):
        egz(k, mz).start()

    xx_finish(NA)
    na_every = na_all[...]
    q_out[...] = mm(na_every, qb_full[...])
    k_out[...] = mm(na_every, kb_full[...])
    v_out[...] = mm(na_every, vb_full[...])
    xx_finish(AL)
    o_out[...] = mm(al_all[...], ctx_full[...])
    for k in range(1, mp):
        egz(k, z_at(-k)).wait_recv()
        summed = summed + egz_all[z_at(-k)].astype(F32)
    eg_out[...] = summed

    for i in range(len(fulls)):
        ag_drain(i, inputs[i] if i < len(inputs) else None)
    for i in range(4):
        xx_drain(i)
    for k in range(1, dp):
        loss_copy(k, me).wait_send()
    for k in range(1, mp):
        for i in range(6):
            rs_copy(i, k, mz, z_at(k)).wait_send()
        for b in range(2):
            zg_copy(6 + b, nh_full, b, k, mz).wait_send()
            zg_copy(8 + b, al_full, b, k, mz).wait_send()
        egz(k, mz).wait_send()
        loss_z(k, mz).wait_send()


def placing_kernel(lift, gains, loss, small, q, k, v, o, h, *outs):
    loss_out, lift_out, gains_out, q_out, k_out, v_out, o_out, h_out = outs
    loss_out[0, 0] = loss[0, 0]
    turned = small[...].T
    lift_out[...] = turned[:lift]
    gains_out[...] = turned[lift : lift + gains]
    q_out[...] = q[...]
    k_out[...] = k[...]
    v_out[...] = v[...]
    o_out[...] = o[...]
    h_out[...] = h[...]


def fused_device(
    dp,
    mp,
    history_sequences,
    later_steps,
    patch_lift_matrix,
    scaling_factors,
    asking_matrix,
    lookup_matrix,
    content_matrix,
    attend_exit_matrix,
    outlook_matrix,
):
    number = history_sequences.shape[0]
    rows = number * PATCHES
    cut, cols = asking_matrix.shape
    width = cut * dp
    small = jnp.concatenate([patch_lift_matrix, scaling_factors], axis=0)
    small = jnp.pad(small, ((0, 128 - small.shape[0]), (0, 0))).T
    vmem = pltpu.VMEM
    full = vmem((width, cols), BF)
    tall = vmem((rows * dp, cols), BF)
    across = vmem((cut, rows * dp), BF)
    dma = pltpu.SemaphoreType.DMA
    grad = jax.ShapeDtypeStruct((cut, cols), F32)
    half = rows // 2
    shard = half // mp
    chips = dp // 2
    results = pl.pallas_call(
        functools.partial(sublayer_kernel, (dp, mp)),
        out_shape=(
            jax.ShapeDtypeStruct((8, 128), F32),
            jax.ShapeDtypeStruct((cut, 128), F32),
            grad, grad, grad, grad, grad,
        ),
        in_specs=[pl.BlockSpec(memory_space=vmem)] * 9,
        out_specs=(pl.BlockSpec(memory_space=vmem),) * 7,
        scratch_shapes=[
            vmem((width, 128), BF), full, full, full, full, full,
            tall, tall, tall, tall, tall,
            vmem((4, width, rows), BF),
            across, across, across,
            vmem((dp, cut, rows), BF),
            vmem((6, half, width), BF),
            vmem((6, mp, shard, width), BF),
            vmem((rows, width), BF),
            vmem((rows, width), BF),
            vmem((rows, width), F32),
            vmem((rows, 128), BF),
            vmem((2, cols // HEAD_DIM, half, half), F32),
            vmem((cut, 128), BF),
            vmem((mp, cut, 128), BF),
            vmem((8, 128), F32),
            vmem((dp, 8, 128), F32),
            vmem((8, 128), F32),
            vmem((mp, 8, 128), F32),
            dma((11, 2 * chips - 1)), dma((11, 2 * chips - 1)),
            dma((4, dp)), dma((4, dp)),
            dma((11, mp)), dma((11, mp)),
            dma((2, max(dp, mp))), dma((2, max(dp, mp))),
        ],
        compiler_params=pltpu.CompilerParams(
            collective_id=0, has_side_effects=True, vmem_limit_bytes=56 * 1024 * 1024
        ),
    )(
        history_sequences, later_steps, small, asking_matrix, lookup_matrix, content_matrix,
        attend_exit_matrix.T, outlook_matrix,
        jnp.asarray(position_table(PATCHES, width)),
    )
    lift = patch_lift_matrix.shape[0]
    gains = scaling_factors.shape[0]
    space = pl.BlockSpec(memory_space=vmem)
    loss, *grads = pl.pallas_call(
        functools.partial(placing_kernel, lift, gains),
        out_shape=(
            jax.ShapeDtypeStruct((1, 1), F32),
            jax.ShapeDtypeStruct((lift, cut), F32),
            jax.ShapeDtypeStruct((gains, cut), F32),
            grad, grad, grad, grad, grad,
        ),
        in_specs=[space] * 7,
        out_specs=(pl.BlockSpec(memory_space=pltpu.SMEM), *([space] * 7)),
    )(*results)
    return (loss.reshape(()), *grads[:5], grads[5].T, grads[6])


def fits(dp, mp, arrays):
    rows = arrays[0].shape[0] * PATCHES
    cut, cols = arrays[4].shape
    return (
        rows == 128
        and dp % 2 == 0
        and dp > 2
        and mp > 1
        and cut % 16 == 0
        and rows % (32 * mp) == 0
        and cols % HEAD_DIM == 0
        and cols == PATCH * LEVEL_CHANNELS
    )


def solution(mesh):
    in_specs = (
        P("dp", None),
        P("dp", None),
        P(None, "dp"),
        P(None, "dp"),
        P("dp", "mp"),
        P("dp", "mp"),
        P("dp", "mp"),
        P("mp", "dp"),
        P("dp", "mp"),
    )
    out_specs = (
        P(),
        P(None, "dp"),
        P(None, "dp"),
        P("dp", "mp"),
        P("dp", "mp"),
        P("dp", "mp"),
        P("mp", "dp"),
        P("dp", "mp"),
    )
    dp, mp = mesh.shape["dp"], mesh.shape["mp"]

    def step(*arrays):
        if fits(dp, mp, arrays):
            return fused_device(dp, mp, *arrays)
        return per_device(*arrays)

    return jax.shard_map(
        step, mesh=mesh, in_specs=in_specs, out_specs=out_specs, check_vma=False
    )
```

```python
import functools
import math

import jax
import jax.numpy as jnp
import numpy as np
from jax import lax
from jax.experimental import pallas as pl
from jax.experimental.pallas import tpu as pltpu
from jax.sharding import PartitionSpec as P

PATCH = 32
HORIZON_SPAN = 128
PATCHES = 16
LEVEL_CHANNELS = 10
HEAD_DIM = 80


EPS = 1e-06
STAT_EPS = 1e-05
SMOOTHING_RADIUS = 0.05


def rms_forward(residual, gain):
    factor = lax.rsqrt(jnp.mean(residual * residual, axis=1, keepdims=True) + EPS)
    return ((residual * factor * gain[None, :]).astype(jnp.bfloat16), factor)


def rms_backward(residual, factor, gain, upstream):
    weighted = gain[None, :] * upstream
    inner = jnp.mean(weighted * residual, axis=1, keepdims=True)
    back = factor * weighted - residual * factor * factor * factor * inner
    gain_term = jnp.sum(upstream * residual * factor, axis=0)
    return (back, gain_term)


def positions(length, width):
    half = width // 2
    freqs = jnp.exp(-math.log(10000.0) * jnp.arange(half, dtype=jnp.float32) / half)
    angles = jnp.arange(length, dtype=jnp.float32)[:, None] * freqs[None, :]
    return jnp.concatenate([jnp.sin(angles), jnp.cos(angles)], axis=1)


def prepare(history_sequences, later_steps):
    number = history_sequences.shape[0]
    centre = jnp.mean(history_sequences, axis=1, keepdims=True)
    spread = jnp.sqrt(
        jnp.mean((history_sequences - centre) * (history_sequences - centre), axis=1, keepdims=True)
        + STAT_EPS
    )
    normed = (history_sequences - centre) / spread
    ahead = (later_steps - centre) / spread
    joined = jnp.concatenate([normed, ahead], axis=1).reshape(number, -1, PATCH)
    reach = later_steps.shape[1] // PATCH
    future_values = jnp.concatenate(
        [joined[:, offset + 1 : offset + 1 + PATCHES] for offset in range(reach)], axis=2
    )
    future_values = future_values.reshape(number * PATCHES, reach * PATCH)
    patches = normed.reshape(number * PATCHES, PATCH).astype(jnp.bfloat16)
    return (patches, future_values)


def attention_forward(queries, keys, values, number):
    layout = (number, PATCHES, -1, HEAD_DIM)
    query_blocks = queries.reshape(layout)
    key_blocks = keys.reshape(layout)
    value_blocks = values.reshape(layout)
    scale = 1.0 / math.sqrt(HEAD_DIM)
    scores = (
        jnp.einsum("sihd,sjhd->shij", query_blocks, key_blocks, preferred_element_type=jnp.float32)
        * scale
    )
    place = jnp.arange(PATCHES)
    causal = place[:, None] >= place[None, :]
    raised = jnp.where(causal, jnp.exp(scores), 0.0)
    probs = raised / jnp.sum(raised, axis=3, keepdims=True)
    probs_low = probs.astype(jnp.bfloat16)
    context = jnp.einsum(
        "shij,sjhd->sihd", probs_low, value_blocks, preferred_element_type=jnp.float32
    )
    context = context.astype(jnp.bfloat16).reshape(number * PATCHES, -1)
    return (context, probs, probs_low)


def attention_backward(context_grad, queries, keys, values, probs, probs_low, number):
    layout = (number, PATCHES, -1, HEAD_DIM)
    query_blocks = queries.reshape(layout)
    key_blocks = keys.reshape(layout)
    value_blocks = values.reshape(layout)
    grad_blocks = context_grad.reshape(layout)
    scale = 1.0 / math.sqrt(HEAD_DIM)
    prob_grad = jnp.einsum(
        "sihd,sjhd->shij", grad_blocks, value_blocks, preferred_element_type=jnp.float32
    )
    value_back = jnp.einsum(
        "shij,sihd->sjhd", probs_low, grad_blocks, preferred_element_type=jnp.float32
    ).astype(jnp.bfloat16)
    centred = prob_grad - jnp.sum(probs * prob_grad, axis=3, keepdims=True)
    score_grad = (probs * centred * scale).astype(jnp.bfloat16)
    query_back = jnp.einsum(
        "shij,sjhd->sihd", score_grad, key_blocks, preferred_element_type=jnp.float32
    ).astype(jnp.bfloat16)
    key_back = jnp.einsum(
        "shij,sihd->sjhd", score_grad, query_blocks, preferred_element_type=jnp.float32
    ).astype(jnp.bfloat16)
    flat = (number * PATCHES, -1)
    return (query_back.reshape(flat), key_back.reshape(flat), value_back.reshape(flat))


def pinball_terms(estimate_entries, actual_entries):
    batch_example_tally = estimate_entries.shape[0]
    horizon_error = actual_entries[:, :, None] - estimate_entries.reshape(
        batch_example_tally, -1, LEVEL_CHANNELS
    )
    cumulative_share = jnp.arange(LEVEL_CHANNELS, dtype=jnp.float32) / LEVEL_CHANNELS
    mean_indicator = jnp.arange(LEVEL_CHANNELS) == 0
    lopsided_errors = jnp.where(
        mean_indicator,
        horizon_error * horizon_error,
        cumulative_share * horizon_error
        + SMOOTHING_RADIUS * jax.nn.softplus(-horizon_error / SMOOTHING_RADIUS),
    )
    skew_coefficient = (
        jnp.where(
            mean_indicator,
            -2.0 * horizon_error,
            jax.nn.sigmoid(-horizon_error / SMOOTHING_RADIUS) - cumulative_share,
        )
        / HORIZON_SPAN
    )
    return (
        jnp.sum(lopsided_errors) / HORIZON_SPAN,
        skew_coefficient.reshape(batch_example_tally, -1).astype(jnp.bfloat16),
    )


def multiplied_rows(left, right):

    def term(start, count):
        return jnp.dot(left, right, preferred_element_type=jnp.float32)

    return term


def per_device(
    history_sequences,
    later_steps,
    patch_lift_matrix,
    scaling_factors,
    asking_matrix,
    lookup_matrix,
    content_matrix,
    attend_exit_matrix,
    outlook_matrix,
):
    number = history_sequences.shape[0]
    rows_all = number * PATCHES
    patches, future_values = prepare(history_sequences, later_steps)
    embed_full, gains_full = (
        lax.all_gather(patch_lift_matrix, "dp", axis=1, tiled=True),
        lax.all_gather(scaling_factors, "dp", axis=1, tiled=True),
    )
    gains = gains_full.astype(jnp.float32)
    query_full, key_full, value_full, outlook_collected = (
        lax.all_gather(asking_matrix, "dp", axis=0, tiled=True),
        lax.all_gather(lookup_matrix, "dp", axis=0, tiled=True),
        lax.all_gather(content_matrix, "dp", axis=0, tiled=True),
        lax.all_gather(outlook_matrix, "dp", axis=0, tiled=True),
    )
    output_full = lax.all_gather(attend_exit_matrix, "dp", axis=1, tiled=True)
    residual_zero = jnp.dot(patches, embed_full, preferred_element_type=jnp.float32) + jnp.tile(
        positions(PATCHES, embed_full.shape[1]), (number, 1)
    )
    normed_attn, factor_attn = rms_forward(residual_zero, gains[0])
    queries = jnp.dot(normed_attn, query_full, preferred_element_type=jnp.float32).astype(
        jnp.bfloat16
    )
    keys = jnp.dot(normed_attn, key_full, preferred_element_type=jnp.float32).astype(jnp.bfloat16)
    values = jnp.dot(normed_attn, value_full, preferred_element_type=jnp.float32).astype(
        jnp.bfloat16
    )
    context, probs, probs_low = attention_forward(queries, keys, values, number)
    attn_term = multiplied_rows(context, output_full)
    residual_one = residual_zero + lax.psum(attn_term(0, rows_all), "mp")
    normed_head, factor_head = rms_forward(residual_one, gains[1])
    estimate_entries = jnp.dot(normed_head, outlook_collected, preferred_element_type=jnp.float32)
    device_portion = estimate_entries.shape[1] // LEVEL_CHANNELS
    actual_entries = lax.dynamic_slice_in_dim(
        future_values, lax.axis_index("mp") * device_portion, device_portion, 1
    )
    device_loss, estimate_derivative = pinball_terms(estimate_entries, actual_entries)
    total_loss_value = lax.psum(device_loss, ("dp", "mp"))
    loss_mean = total_loss_value / (number * PATCHES * lax.axis_size("dp"))
    head_weight_gradient = jnp.dot(
        normed_head.T, estimate_derivative, preferred_element_type=jnp.float32
    )
    head_contribution = multiplied_rows(estimate_derivative, outlook_collected.T)
    head_reverse = lax.psum(head_contribution(0, rows_all).astype(jnp.bfloat16), "mp").astype(
        jnp.float32
    )
    residual_one_grad, gain_one = rms_backward(residual_one, factor_head, gains[1], head_reverse)
    attn_low = residual_one_grad.astype(jnp.bfloat16)
    output_grad = jnp.dot(context.T, attn_low, preferred_element_type=jnp.float32)
    context_grad = jnp.dot(attn_low, output_full.T, preferred_element_type=jnp.float32).astype(
        jnp.bfloat16
    )
    query_back, key_back, value_back = attention_backward(
        context_grad, queries, keys, values, probs, probs_low, number
    )
    query_grad = jnp.dot(normed_attn.T, query_back, preferred_element_type=jnp.float32)
    key_grad = jnp.dot(normed_attn.T, key_back, preferred_element_type=jnp.float32)
    value_grad = jnp.dot(normed_attn.T, value_back, preferred_element_type=jnp.float32)
    total = jnp.dot(query_back, query_full.T, preferred_element_type=jnp.float32)
    total = total + jnp.dot(key_back, key_full.T, preferred_element_type=jnp.float32)
    attn_back = lax.psum(
        (total + jnp.dot(value_back, value_full.T, preferred_element_type=jnp.float32)).astype(
            jnp.bfloat16
        ),
        "mp",
    ).astype(jnp.float32)
    norm_back_zero, gain_zero = rms_backward(residual_zero, factor_attn, gains[0], attn_back)
    residual_zero_grad = residual_one_grad + norm_back_zero
    embed_grad = jnp.dot(
        patches.T, residual_zero_grad.astype(jnp.bfloat16), preferred_element_type=jnp.float32
    )
    gains_grad = jnp.stack([gain_zero, gain_one], axis=0)
    query_grad, key_grad, value_grad, head_weight_gradient = (
        lax.psum_scatter(query_grad, "dp", scatter_dimension=0, tiled=True),
        lax.psum_scatter(key_grad, "dp", scatter_dimension=0, tiled=True),
        lax.psum_scatter(value_grad, "dp", scatter_dimension=0, tiled=True),
        lax.psum_scatter(head_weight_gradient, "dp", scatter_dimension=0, tiled=True),
    )
    output_grad = lax.psum_scatter(output_grad, "dp", scatter_dimension=1, tiled=True)
    embed_grad, gains_grad = (
        lax.psum_scatter(embed_grad, "dp", scatter_dimension=1, tiled=True),
        lax.psum_scatter(gains_grad, "dp", scatter_dimension=1, tiled=True),
    )
    return (
        loss_mean,
        embed_grad,
        gains_grad,
        query_grad,
        key_grad,
        value_grad,
        output_grad,
        head_weight_gradient,
    )


MESH = pl.DeviceIdType.MESH
BF = jnp.bfloat16
F32 = jnp.float32


def mm(left, right, dims=(1, 0)):
    return lax.dot_general(
        left, right, (((dims[0],), (dims[1],)), ((), ())), preferred_element_type=F32
    )


def position_table(length, width):
    half = width // 2
    freqs = np.exp(-math.log(10000.0) * np.arange(half, dtype=np.float32) / np.float32(half))
    angles = np.arange(length, dtype=np.float32)[:, None] * freqs.astype(np.float32)[None, :]
    return np.concatenate([np.sin(angles), np.cos(angles)], axis=1).astype(np.float32)


EG, WQ, WK, WV, WO, WH, CTX, FG, QB, KB, VB = range(11)
NA, NH, AL, EP = range(4)


def sublayer_kernel(
    sizes,
    hist,
    later,
    eg_in,
    wq_in,
    wk_in,
    wv_in,
    wo_in,
    wh_in,
    pos,
    loss_out,
    eg_out,
    q_out,
    k_out,
    v_out,
    o_out,
    h_out,
    eg_full,
    wq_full,
    wk_full,
    wv_full,
    wo_full,
    wh_full,
    ctx_full,
    fg_full,
    qb_full,
    kb_full,
    vb_full,
    turned,
    na_all,
    nh_all,
    al_all,
    ep_all,
    parts,
    parts_in,
    nh_full,
    al_full,
    rz_ref,
    patch_ref,
    probs_ref,
    egz_own,
    egz_all,
    loss_own,
    loss_dp,
    loss_mid,
    loss_mp,
    ag_send,
    ag_recv,
    xx_send,
    xx_recv,
    z_send,
    z_recv,
    l_send,
    l_recv,
):
    dp, mp = sizes
    chips = dp // 2
    me = lax.axis_index("dp")
    mz = lax.axis_index("mp")
    core = lax.rem(me, 2)
    chip = me // 2
    twin = chip * 2 + 1 - core
    number, steps = hist.shape
    rows = number * PATCHES
    width = pos.shape[1]
    cut = width // dp
    half = rows // 2
    shard = half // mp
    cols = wq_in.shape[1]
    heads = cols // HEAD_DIM

    def rotated(k):
        return lax.rem(me + k, dp)

    def chip_at(k):
        return lax.rem(chip + k + chips, chips) * 2 + core

    barrier = pltpu.get_barrier_semaphore()
    for k in range(1, dp):
        pl.semaphore_signal(barrier, inc=1, device_id=(rotated(k), mz), device_id_type=MESH)
    for k in range(1, mp):
        pl.semaphore_signal(
            barrier, inc=1, device_id=(me, lax.rem(mz + k, mp)), device_id_type=MESH
        )
    pl.semaphore_wait(barrier, dp - 1 + mp - 1)

    fulls = [
        eg_full, wq_full, wk_full, wv_full, wo_full, wh_full,
        ctx_full, fg_full, qb_full, kb_full, vb_full,
    ]

    def block(full, owner):
        size = full.shape[0] // dp
        return full.at[pl.ds(pl.multiple_of(owner * size, 16), size), :]

    def remote(src, dst, send, recv, device):
        return pltpu.make_async_remote_copy(
            src_ref=src, dst_ref=dst, send_sem=send, recv_sem=recv,
            device_id=device, device_id_type=MESH,
        )

    def ag_copy(i, slot, owner, target, src=None):
        place = block(fulls[i], owner)
        return remote(
            place if src is None else src, place,
            ag_send.at[i, slot], ag_recv.at[i, slot], (target, mz),
        )

    def ag_start(i, src=None):
        for k in range(1, chips):
            ag_copy(i, k, me, chip_at(k), src).start()
        ag_copy(i, 0, me, twin, src).start()

    def ag_finish(i):
        for k in range(1, chips):
            owner = chip_at(-k)
            ag_copy(i, k, owner, twin).wait_recv()
            ag_copy(i, chips - 1 + k, owner, twin).start()
        ag_copy(i, 0, twin, twin).wait_recv()
        for k in range(1, chips):
            other = lax.rem(chip - k + chips, chips) * 2 + 1 - core
            ag_copy(i, chips - 1 + k, other, twin).wait_recv()

    def ag_drain(i, src=None):
        for k in range(1, chips):
            ag_copy(i, k, me, chip_at(k), src).wait_send()
            ag_copy(i, chips - 1 + k, chip_at(-k), twin).wait_send()
        ag_copy(i, 0, me, twin, src).wait_send()

    def store_own(i, value):
        size = fulls[i].shape[0] // dp
        fulls[i][pl.ds(pl.multiple_of(me * size, 16), size), :] = value

    lands = [na_all, nh_all, al_all, ep_all]

    def xx_copy(i, k, sender, target):
        if i == EP:
            dst = ep_all.at[sender]
        else:
            dst = lands[i].at[:, pl.ds(pl.multiple_of(sender * rows, 128), rows)]
        return remote(
            turned.at[i, pl.ds(pl.multiple_of(target * cut, 16), cut), :], dst,
            xx_send.at[i, k], xx_recv.at[i, k], (target, mz),
        )

    def xx_start(i, value):
        turned[i] = value
        for k in range(1, dp):
            xx_copy(i, k, me, rotated(k)).start()
        own = turned[i, pl.ds(pl.multiple_of(me * cut, 16), cut), :]
        if i == EP:
            ep_all[me] = own
        else:
            lands[i][:, pl.ds(pl.multiple_of(me * rows, 128), rows)] = own

    def xx_finish(i):
        for k in range(1, dp):
            xx_copy(i, k, lax.rem(me - k + dp, dp), rotated(k)).wait_recv()

    def xx_drain(i):
        for k in range(1, dp):
            xx_copy(i, k, me, rotated(k)).wait_send()

    def z_at(k):
        return lax.rem(mz + k + mp, mp)

    def rs_copy(i, k, sender, target):
        return remote(
            parts.at[i, pl.ds(pl.multiple_of(target * shard, 16), shard), :],
            parts_in.at[i, sender],
            z_send.at[i, k], z_recv.at[i, k], (me, target),
        )

    def rs_start(i, value):
        parts[i] = value.astype(BF)
        for k in range(1, mp):
            rs_copy(i, k, mz, z_at(k)).start()

    def rs_finish(i):
        total = parts[i, pl.ds(pl.multiple_of(mz * shard, 16), shard), :].astype(F32)
        for k in range(1, mp):
            rs_copy(i, k, z_at(-k), z_at(k)).wait_recv()
            total = total + parts_in[i, z_at(-k)].astype(F32)
        return total

    def held(b, owner):
        return pl.ds(pl.multiple_of(b * half + owner * shard, 16), shard)

    def zg_copy(i, full, b, k, owner):
        place = full.at[held(b, owner), :]
        return remote(place, place, z_send.at[i, k], z_recv.at[i, k], (me, z_at(k)))

    def zg(i, full, b, value):
        full[held(b, mz), :] = value
        for k in range(1, mp):
            zg_copy(i, full, b, k, mz).start()

    def zg_finish(i, full, b):
        for k in range(1, mp):
            zg_copy(i, full, b, k, z_at(-k)).wait_recv()
        return full[b * half : (b + 1) * half, :]

    inputs = [eg_in, wq_in, wk_in, wv_in, wo_in, wh_in]
    for i, ref in enumerate(inputs):
        ag_start(i, ref)
    for i, ref in enumerate(inputs):
        store_own(i, ref[...])

    history = hist[...]
    centre = jnp.mean(history, axis=1, keepdims=True)
    spread = jnp.sqrt(
        jnp.mean((history - centre) * (history - centre), axis=1, keepdims=True) + STAT_EPS
    )
    normed = (history - centre) / spread
    ahead = (later[...] - centre) / spread
    joined = jnp.concatenate([normed, ahead], axis=1)
    span = joined.shape[1]
    wide = jnp.broadcast_to(joined[:, None, :], (number, PATCHES, span)).reshape(rows, span)
    row = lax.broadcasted_iota(jnp.int32, (rows, span), 0)
    at = lax.broadcasted_iota(jnp.int32, (rows, span), 1)
    offset = at - PATCH * (row & (PATCHES - 1))
    here = (offset >= 0) & (offset < PATCH)
    lane = lax.broadcasted_iota(jnp.int32, (span, 128), 1)
    low = lax.broadcasted_iota(jnp.int32, (span, 128), 0) & (PATCH - 1)
    fold = jnp.where(lane == low, 1.0, 0.0).astype(BF)
    patches = mm(jnp.where(here, wide, 0.0).astype(BF), fold).astype(BF)
    patch_ref[...] = patches

    portion = cols // LEVEL_CHANNELS
    reach = offset - PATCH - portion * mz
    chosen = jnp.where((reach >= 0) & (reach < portion), wide, 0.0)
    column = lax.broadcasted_iota(jnp.int32, (span, cols), 1)
    first = (lax.broadcasted_iota(jnp.int32, (span, cols), 0) & (PATCH - 1)) * LEVEL_CHANNELS
    spreader = jnp.where((column >= first) & (column < first + LEVEL_CHANNELS), 1.0, 0.0).astype(BF)
    target = jnp.zeros((rows, cols), F32)
    rest = chosen
    for _ in range(3):
        piece = rest.astype(BF)
        target = target + mm(piece, spreader)
        rest = rest - piece.astype(F32)

    ag_finish(EG)
    lifted = eg_full[...]
    table = jnp.broadcast_to(pos[...][None], (number, PATCHES, width)).reshape(rows, width)
    rz = mm(patches, lifted, (1, 1)) + table
    rz_ref[...] = rz
    pick = lax.broadcasted_iota(jnp.int32, (16, 128), 1) - lax.broadcasted_iota(
        jnp.int32, (16, 128), 0
    )
    gains = mm(jnp.where(pick == PATCH, 1.0, 0.0).astype(BF), lifted, (1, 1))
    gain_attn = gains[0:1, :]
    gain_head = gains[1:2, :]
    factor = lax.rsqrt(jnp.mean(rz * rz, axis=1, keepdims=True) + EPS)
    na = rz * factor * gain_attn
    na_low = na.astype(BF)
    xx_start(NA, na.T.astype(BF))

    ag_finish(WQ)
    q = mm(na_low, wq_full[...])
    ag_finish(WK)
    k_ = mm(na_low, wk_full[...])
    ag_finish(WV)
    v = mm(na_low, wv_full[...])
    q_low, k_low, v_low = q.astype(BF), k_.astype(BF), v.astype(BF)

    head_lane = lax.broadcasted_iota(jnp.int32, (1, cols), 1)
    masks = [
        jnp.where((head_lane >= h * HEAD_DIM) & (head_lane < (h + 1) * HEAD_DIM), 1.0, 0.0)
        for h in range(heads)
    ]
    r_at = lax.broadcasted_iota(jnp.int32, (half, half), 0)
    c_at = lax.broadcasted_iota(jnp.int32, (half, half), 1)
    causal = (c_at <= r_at) & (c_at >= r_at - (r_at & (PATCHES - 1)))
    scale = 1.0 / math.sqrt(HEAD_DIM)
    spans = [slice(b * half, (b + 1) * half) for b in range(2)]
    contexts = []
    for b, span_b in enumerate(spans):
        ctx = jnp.zeros((half, cols), F32)
        for h in range(heads):
            q_head = (q[span_b] * masks[h]).astype(BF)
            scores = mm(q_head, k_low[span_b], (1, 1)) * scale
            raised = jnp.where(causal, jnp.exp(scores), 0.0)
            probs = raised / jnp.sum(raised, axis=1, keepdims=True)
            probs_ref[b, h] = probs
            ctx = ctx + mm(probs.astype(BF), (v[span_b] * masks[h]).astype(BF))
        contexts.append(ctx.astype(BF))
        if b == 0:
            ag_finish(WO)
        rs_start(b, mm(contexts[b], wo_full[...], (1, 1)))
    store_own(CTX, jnp.concatenate(contexts, axis=0))
    ag_start(CTX)
    rz_shards, r1s, factors = [], [], []
    for b in range(2):
        rz_shards.append(rz_ref[held(b, mz), :])
        r1 = rz_shards[b] + rs_finish(b)
        factor_head = lax.rsqrt(jnp.mean(r1 * r1, axis=1, keepdims=True) + EPS)
        zg(6 + b, nh_full, b, (r1 * factor_head * gain_head).astype(BF))
        r1s.append(r1)
        factors.append(factor_head)
    ag_finish(WH)
    level = lax.broadcasted_iota(jnp.int32, (1, cols), 1).astype(F32)
    level = level - LEVEL_CHANNELS * jnp.floor((level + 0.5) / LEVEL_CHANNELS)
    shares = level / LEVEL_CHANNELS
    is_mean = shares == 0.0
    terms = jnp.zeros((half, cols), F32)
    slopes = []
    for b, span_b in enumerate(spans):
        nh = zg_finish(6 + b, nh_full, b)
        error = target[span_b] - mm(nh, wh_full[...])
        slope = -error / SMOOTHING_RADIUS
        small = jnp.exp(-jnp.abs(slope))
        soft = jnp.maximum(slope, 0.0) + jnp.log1p(small)
        sig = jnp.where(slope >= 0.0, 1.0, small) / (1.0 + small)
        terms = terms + jnp.where(
            is_mean, error * error, shares * error + SMOOTHING_RADIUS * soft
        )
        fg = (jnp.where(is_mean, -2.0 * error, sig - shares) / HORIZON_SPAN).astype(BF)
        slopes.append(fg)
        rs_start(2 + b, mm(fg, wh_full[...], (1, 1)))
    store_own(FG, jnp.concatenate(slopes, axis=0))
    ag_start(FG)
    xx_start(NH, nh_full[...].astype(F32).T.astype(BF))
    loss_here = jnp.sum(jnp.sum(terms, axis=1, keepdims=True), axis=0, keepdims=True)
    loss_own[...] = jnp.broadcast_to(loss_here, loss_own.shape)

    def loss_copy(k, sender):
        return remote(
            loss_own, loss_dp.at[sender], l_send.at[0, k], l_recv.at[0, k], (rotated(k), mz)
        )

    def loss_z(k, sender):
        return remote(
            loss_mid, loss_mp.at[sender], l_send.at[1, k], l_recv.at[1, k], (me, z_at(k))
        )

    for k in range(1, dp):
        loss_copy(k, me).start()
    ag_finish(CTX)

    r1_grads = []
    gain_one = jnp.zeros((1, width), F32)
    for b in range(2):
        up = rs_finish(2 + b)
        r1, factor_head = r1s[b], factors[b]
        weighted = gain_head * up
        inner = jnp.mean(weighted * r1, axis=1, keepdims=True)
        r1_grad = factor_head * weighted - r1 * factor_head * factor_head * factor_head * inner
        zg(8 + b, al_full, b, r1_grad.astype(BF))
        r1_grads.append(r1_grad)
        gain_one = gain_one + jnp.sum(up * r1 * factor_head, axis=0, keepdims=True)
    backs = []
    for b, span_b in enumerate(spans):
        al = zg_finish(8 + b, al_full, b)
        if b == 1:
            xx_start(AL, al_full[...].astype(F32).T.astype(BF))
        cg = mm(al, wo_full[...])
        qb = jnp.zeros((half, cols), F32)
        kb = jnp.zeros((half, cols), F32)
        vb = jnp.zeros((half, cols), F32)
        for h in range(heads):
            cg_head = (cg * masks[h]).astype(BF)
            probs = probs_ref[b, h]
            prob_grad = mm(cg_head, v_low[span_b], (1, 1))
            vb = vb + mm(probs.T.astype(BF), cg_head)
            centred = prob_grad - jnp.sum(probs * prob_grad, axis=1, keepdims=True)
            score_grad = probs * centred * scale
            qb = qb + mm(score_grad.astype(BF), (k_[span_b] * masks[h]).astype(BF))
            kb = kb + mm(score_grad.T.astype(BF), (q[span_b] * masks[h]).astype(BF))
        qb, kb, vb = qb.astype(BF), kb.astype(BF), vb.astype(BF)
        backs.append((qb, kb, vb))
        back = mm(qb, wq_full[...], (1, 1)) + mm(kb, wk_full[...], (1, 1))
        rs_start(4 + b, back + mm(vb, wv_full[...], (1, 1)))
    for n, i in enumerate((QB, KB, VB)):
        store_own(i, jnp.concatenate([backs[0][n], backs[1][n]], axis=0))
        ag_start(i)
    ag_finish(FG)

    total = loss_own[...]
    for k in range(1, dp):
        loss_copy(k, lax.rem(me - k + dp, dp)).wait_recv()
        total = total + loss_dp[lax.rem(me - k + dp, dp)]
    loss_mid[...] = total
    for k in range(1, mp):
        loss_z(k, mz).start()
    xx_finish(NH)
    h_out[...] = mm(nh_all[...], fg_full[...])

    rz_grads = []
    gain_zero = jnp.zeros((1, width), F32)
    for b in range(2):
        up = rs_finish(4 + b)
        rz_shard = rz_shards[b]
        factor = lax.rsqrt(jnp.mean(rz_shard * rz_shard, axis=1, keepdims=True) + EPS)
        weighted = gain_attn * up
        inner = jnp.mean(weighted * rz_shard, axis=1, keepdims=True)
        rz_grads.append(
            r1_grads[b] + (factor * weighted - rz_shard * factor * factor * factor * inner)
        )
        gain_zero = gain_zero + jnp.sum(up * rz_shard * factor, axis=0, keepdims=True)
    which = lax.broadcasted_iota(jnp.int32, (16, width), 0)
    both = jnp.where(which == 0, gain_zero, jnp.where(which == 1, gain_one, 0.0))
    both_high = both.astype(BF).astype(F32)
    stacked = jnp.concatenate([*rz_grads, both_high, both - both_high], axis=0)
    hot = jnp.where(pick == PATCH, 1.0, 0.0)
    mine = [patch_ref[held(b, mz), :].astype(F32) for b in range(2)]
    other = jnp.concatenate([*mine, hot, hot], axis=0)
    xx_start(EP, mm(stacked.T.astype(BF), other.astype(BF)).astype(BF))

    total = loss_mid[...]
    for k in range(1, mp):
        loss_z(k, z_at(-k)).wait_recv()
        total = total + loss_mp[z_at(-k)]
    loss_out[...] = total / (number * PATCHES * dp * HORIZON_SPAN)
    for i in (QB, KB, VB):
        ag_finish(i)

    xx_finish(EP)
    summed = ep_all[0].astype(F32)
    for d in range(1, dp):
        summed = summed + ep_all[d].astype(F32)
    egz_own[...] = summed.astype(BF)

    def egz(k, sender):
        return remote(egz_own, egz_all.at[sender], z_send.at[10, k], z_recv.at[10, k], (me, z_at(k)))

    for k in range(1, mp):
        egz(k, mz).start()

    xx_finish(NA)
    na_every = na_all[...]
    q_out[...] = mm(na_every, qb_full[...])
    k_out[...] = mm(na_every, kb_full[...])
    v_out[...] = mm(na_every, vb_full[...])
    xx_finish(AL)
    o_out[...] = mm(al_all[...], ctx_full[...])
    for k in range(1, mp):
        egz(k, z_at(-k)).wait_recv()
        summed = summed + egz_all[z_at(-k)].astype(F32)
    eg_out[...] = summed

    for i in range(len(fulls)):
        ag_drain(i, inputs[i] if i < len(inputs) else None)
    for i in range(4):
        xx_drain(i)
    for k in range(1, dp):
        loss_copy(k, me).wait_send()
    for k in range(1, mp):
        for i in range(6):
            rs_copy(i, k, mz, z_at(k)).wait_send()
        for b in range(2):
            zg_copy(6 + b, nh_full, b, k, mz).wait_send()
            zg_copy(8 + b, al_full, b, k, mz).wait_send()
        egz(k, mz).wait_send()
        loss_z(k, mz).wait_send()


def placing_kernel(lift, gains, loss, small, q, k, v, o, h, *outs):
    loss_out, lift_out, gains_out, q_out, k_out, v_out, o_out, h_out = outs
    loss_out[0, 0] = loss[0, 0]
    turned = small[...].T
    lift_out[...] = turned[:lift]
    gains_out[...] = turned[lift : lift + gains]
    q_out[...] = q[...]
    k_out[...] = k[...]
    v_out[...] = v[...]
    o_out[...] = o[...]
    h_out[...] = h[...]


def fused_device(
    dp,
    mp,
    history_sequences,
    later_steps,
    patch_lift_matrix,
    scaling_factors,
    asking_matrix,
    lookup_matrix,
    content_matrix,
    attend_exit_matrix,
    outlook_matrix,
):
    number = history_sequences.shape[0]
    rows = number * PATCHES
    cut, cols = asking_matrix.shape
    width = cut * dp
    small = jnp.concatenate([patch_lift_matrix, scaling_factors], axis=0)
    small = jnp.pad(small, ((0, 128 - small.shape[0]), (0, 0))).T
    vmem = pltpu.VMEM
    full = vmem((width, cols), BF)
    tall = vmem((rows * dp, cols), BF)
    across = vmem((cut, rows * dp), BF)
    dma = pltpu.SemaphoreType.DMA
    grad = jax.ShapeDtypeStruct((cut, cols), F32)
    half = rows // 2
    shard = half // mp
    chips = dp // 2
    results = pl.pallas_call(
        functools.partial(sublayer_kernel, (dp, mp)),
        out_shape=(
            jax.ShapeDtypeStruct((8, 128), F32),
            jax.ShapeDtypeStruct((cut, 128), F32),
            grad, grad, grad, grad, grad,
        ),
        in_specs=[pl.BlockSpec(memory_space=vmem)] * 9,
        out_specs=(pl.BlockSpec(memory_space=vmem),) * 7,
        scratch_shapes=[
            vmem((width, 128), BF), full, full, full, full, full,
            tall, tall, tall, tall, tall,
            vmem((4, width, rows), BF),
            across, across, across,
            vmem((dp, cut, rows), BF),
            vmem((6, half, width), BF),
            vmem((6, mp, shard, width), BF),
            vmem((rows, width), BF),
            vmem((rows, width), BF),
            vmem((rows, width), F32),
            vmem((rows, 128), BF),
            vmem((2, cols // HEAD_DIM, half, half), F32),
            vmem((cut, 128), BF),
            vmem((mp, cut, 128), BF),
            vmem((8, 128), F32),
            vmem((dp, 8, 128), F32),
            vmem((8, 128), F32),
            vmem((mp, 8, 128), F32),
            dma((11, 2 * chips - 1)), dma((11, 2 * chips - 1)),
            dma((4, dp)), dma((4, dp)),
            dma((11, mp)), dma((11, mp)),
            dma((2, max(dp, mp))), dma((2, max(dp, mp))),
        ],
        compiler_params=pltpu.CompilerParams(
            collective_id=0, has_side_effects=True, vmem_limit_bytes=56 * 1024 * 1024
        ),
    )(
        history_sequences, later_steps, small, asking_matrix, lookup_matrix, content_matrix,
        attend_exit_matrix.T, outlook_matrix,
        jnp.asarray(position_table(PATCHES, width)),
    )
    lift = patch_lift_matrix.shape[0]
    gains = scaling_factors.shape[0]
    space = pl.BlockSpec(memory_space=vmem)
    loss, *grads = pl.pallas_call(
        functools.partial(placing_kernel, lift, gains),
        out_shape=(
            jax.ShapeDtypeStruct((1, 1), F32),
            jax.ShapeDtypeStruct((lift, cut), F32),
            jax.ShapeDtypeStruct((gains, cut), F32),
            grad, grad, grad, grad, grad,
        ),
        in_specs=[space] * 7,
        out_specs=(pl.BlockSpec(memory_space=pltpu.SMEM), *([space] * 7)),
    )(*results)
    return (loss.reshape(()), *grads[:5], grads[5].T, grads[6])


def fits(dp, mp, arrays):
    rows = arrays[0].shape[0] * PATCHES
    cut, cols = arrays[4].shape
    return (
        rows == 128
        and dp % 2 == 0
        and dp > 2
        and mp > 1
        and cut % 16 == 0
        and rows % (32 * mp) == 0
        and cols % HEAD_DIM == 0
        and cols == PATCH * LEVEL_CHANNELS
    )


def solution(mesh):
    in_specs = (
        P("dp", None),
        P("dp", None),
        P(None, "dp"),
        P(None, "dp"),
        P("dp", "mp"),
        P("dp", "mp"),
        P("dp", "mp"),
        P("mp", "dp"),
        P("dp", "mp"),
    )
    out_specs = (
        P(),
        P(None, "dp"),
        P(None, "dp"),
        P("dp", "mp"),
        P("dp", "mp"),
        P("dp", "mp"),
        P("mp", "dp"),
        P("dp", "mp"),
    )
    dp, mp = mesh.shape["dp"], mesh.shape["mp"]

    def step(*arrays):
        if fits(dp, mp, arrays):
            return fused_device(dp, mp, *arrays)
        return per_device(*arrays)

    return jax.shard_map(
        step, mesh=mesh, in_specs=in_specs, out_specs=out_specs, check_vma=False
    )
```
